128 devices in a mesh: member: 8 (over y, core), region: 16 (over x, z).
Axes of the slice: x: 4, y: 4, z: 4, core: 2. Of those that a mesh axis runs over, the one named last changes fastest.
Arguments:
- state: float32 [256, 8, 16384], P('member', None, 'region'), may hold values from -6 to 6
- adjacent_columns: int32 [6, 16384], P(None, 'region'), may hold values from 0 to 16383, as said below
- adjacent_rates: float32 [6, 16384], P(None, 'region'), may hold values from 0.02 to 0.16
- amplification_speed: float32 [16384], P('region'), may hold values from 0.05 to 0.5
- obs_patch: int32 [32768], P(('member', 'region')), may hold values from -1 to 127, as said below
- obs_row: int32 [32768], P(('member', 'region')), may hold values from 0 to 1023
- obs_value: float32 [32768], P(('member', 'region')), may hold values from -6 to 6
- obs_error: float32 [32768], P(('member', 'region')), may hold values from 0.5 to 2
Outputs:
- analysis: bfloat16 [256, 8, 16384], P('member', None, 'region')
The draws below stay inside these ranges and needn't reach their ends.
Inputs may be any that keep to these rules, and one draw needn't show every extreme that they name: `adjacent_columns`: each neighbour lies within 256 positions of its column along the closed order of columns (index modulo 16384) and is never the column itself. `obs_patch`: at most 256 rows name one patch. Within the 256 rows of one device, at most 2 rows name any one patch; -1 marks a row without an observation.
All inputs are finite; a program needn't handle non-finite values.
Results may differ from the reference program's by a relative error of at most 0.01.
Values may be sent and summed in bfloat16 or wider, within the bound.
No kernel may reach another device: no remote copies, remote signals or barrier semaphores. Data moves between devices by JAX's collectives and lax.ppermute only.
A program may use at most 64 MiB of HBM per device.

```python
import math
import jax
import jax.numpy as jnp
from jax import lax

LEVELS = 8
PATCH_CELLS = 128
PATCH_DEV = 1
PATCH_OBS = 256
RIM = 256
STEPS = 3
NS_ITERS = 6
MEMBERS = 256
CELL_DEV = 1024
CELLS = 16384
PATCHES = 128
OBS_TOTAL = 32768
N_MEMBER = 8
N_REGION = 16


def draw_adjacent_columns(key, part):
    cells_all = CELL_DEV * N_REGION
    cell_index = jnp.arange(cells_all, dtype=jnp.int32)
    stride = jax.random.randint(jax.random.fold_in(key, 11), (6, cells_all), 1, RIM + 1)
    flips = jax.random.randint(jax.random.fold_in(key, 12), (6, cells_all), 0, 2)
    offsets = jnp.where(flips == 0, -stride, stride)
    offsets = offsets.at[0].set(jnp.where(cell_index % CELL_DEV == 0, -RIM, offsets[0]))
    offsets = offsets.at[1].set(jnp.where(cell_index % CELL_DEV == CELL_DEV - 1, RIM, offsets[1]))
    return ((cell_index[None, :] + offsets) % cells_all).astype(jnp.int32)


def draw_obs_patch(key, part):
    devices = N_MEMBER * N_REGION
    observation_shard = PATCH_DEV * PATCH_OBS
    total_rows = devices * observation_shard
    slot_position = jnp.arange(total_rows, dtype=jnp.int32)
    target = slot_position // observation_shard
    within = slot_position % observation_shard
    local_patch = within // PATCH_OBS
    shifts = jax.random.randint(jax.random.fold_in(key, 21), (devices,), 0, devices)
    source = (within + shifts[target]) % devices
    region_of = target % N_REGION
    member_of = target // N_REGION
    patch_id = region_of * (N_MEMBER * PATCH_DEV) + member_of * PATCH_DEV + local_patch
    levels_raw = jax.random.randint(jax.random.fold_in(key, 22), (devices * PATCH_DEV,), 0, 1001)
    fill_level = 100 + 900 * levels_raw * levels_raw // 1000000
    full_device = jax.random.randint(jax.random.fold_in(key, 23), (), 0, devices)
    slot_fill = jnp.where(target == full_device, 1001, fill_level[target * PATCH_DEV + local_patch])
    draws_live = jax.random.randint(jax.random.fold_in(key, 24), (total_rows,), 0, 1000)
    labelled = jnp.where(draws_live < slot_fill, patch_id, -1)
    shuffle = jax.random.permutation(jax.random.fold_in(key, 25), total_rows).astype(jnp.int32)
    ordering = jnp.argsort(source * total_rows + shuffle, stable=True)
    return labelled[ordering].astype(jnp.int32)


def set_ends(result, key, low, high):
    longest = result.shape.index(max(result.shape))
    spots = []
    for shift in (0, 1):
        where = [jax.random.randint(jax.random.fold_in(key, axis), (), 0, length) for axis, length in enumerate(result.shape)]
        where[longest] = (where[longest] + shift) % result.shape[longest]
        spots.append(tuple(where))
    return result.at[spots[0]].set(low).at[spots[1]].set(high)


def shard_levels(rng, extent, split, low, top_value):
    def one(position, shards_of):
        heights = jax.random.uniform(jax.random.fold_in(jax.random.fold_in(rng, 6), position), (shards_of,), jnp.float32, low / len(split), top_value / len(split))
        return jnp.repeat(jnp.exp(heights), extent[position] // shards_of).reshape((-1,) + (1,) * (len(extent) - position - 1))

    factor_of = one(*split[0])
    for cut in split[1:]:
        factor_of = factor_of * one(*cut)
    return factor_of


def centred(rng, shape, scale, reach, cuts=(), held_as=jnp.bfloat16):
    array = scale * jax.random.normal(rng, shape, jnp.float32)
    if cuts:
        array = array * shard_levels(rng, shape, cuts, -0.22, 0.18)
    return jnp.clip(array, -reach, reach).astype(held_as)


def setup_inputs(seed: int = 0) -> dict:
    arg_keys = jax.random.split(jax.random.key(seed), 9)
    state = centred(arg_keys[0], (MEMBERS, LEVELS, CELLS), 1.0, 6.0, ((0, 8), (2, 16)), jnp.float32)
    adjacent_columns = draw_adjacent_columns(jax.random.fold_in(arg_keys[8], 71), 0)
    adjacent_rates = jnp.clip(0.02 + 0.14 * jax.random.uniform(arg_keys[2], (6, CELLS), jnp.float32) ** shard_levels(arg_keys[2], (6, CELLS), ((1, 16),), -0.2, 0.2), 0.02, 0.16)
    amplification_speed = jnp.clip(jnp.exp(math.log(0.5) - 2.3025851 * jax.random.uniform(arg_keys[3], (CELLS,), jnp.float32) ** shard_levels(arg_keys[3], (CELLS,), ((0, 16),), -0.2, 0.2)), 0.05, 0.5)
    obs_patch = draw_obs_patch(jax.random.fold_in(arg_keys[8], 71), 0)
    obs_row = set_ends(jax.random.randint(arg_keys[5], (OBS_TOTAL,), 0, LEVELS * PATCH_CELLS), jax.random.fold_in(arg_keys[5], 1), 0, (LEVELS * PATCH_CELLS) - 1).astype(jnp.int32)
    obs_value = centred(arg_keys[6], (OBS_TOTAL,), 1.0, 6.0, ((0, 128),), jnp.float32)
    obs_error = jnp.clip(jnp.exp(math.log(2.0) - 1.3862944 * jax.random.uniform(arg_keys[7], (OBS_TOTAL,), jnp.float32) ** shard_levels(arg_keys[7], (OBS_TOTAL,), ((0, 128),), -0.2, 0.2)), 0.5, 2.0)
    return dict(state=state, adjacent_columns=adjacent_columns, adjacent_rates=adjacent_rates, amplification_speed=amplification_speed, obs_patch=obs_patch, obs_row=obs_row, obs_value=obs_value, obs_error=obs_error)


def propagate_prediction(model_variable_array, adjacent_columns, adjacent_rates, amplification_speed):
    summed = jnp.zeros_like(model_variable_array)
    for neighbour in range(6):
        summed = summed + adjacent_rates[neighbour] * (jnp.take(model_variable_array, adjacent_columns[neighbour], axis=2) - model_variable_array)
    blended = model_variable_array + summed
    return blended + amplification_speed * jnp.tanh(blended)

def analyse(ensemble_realizations, row_index, values, weight_matrix):
    ensemble = ensemble_realizations.shape[0]
    average = lax.optimization_barrier(jnp.mean(ensemble_realizations, axis=0))
    anomaly = ensemble_realizations - average[None, :]
    observed = jnp.take(anomaly, row_index, axis=1)
    innovation = values - jnp.take(average, row_index)
    rooted = jnp.sqrt(weight_matrix)
    spread = math.sqrt(ensemble - 1.0)
    scaled = observed * rooted[None, :] / spread
    identity = jnp.eye(ensemble, dtype=jnp.float32)
    system = identity + jnp.dot(scaled, scaled.T, precision=lax.Precision.HIGHEST)
    norm_fro = jnp.sqrt(jnp.sum(system * system))
    iterate = system / norm_fro
    inverse_root = identity
    for sweep in range(NS_ITERS):
        factor = 1.5 * identity - 0.5 * jnp.dot(inverse_root, iterate, precision=lax.Precision.HIGHEST)
        iterate = jnp.dot(iterate, factor, precision=lax.Precision.HIGHEST)
        inverse_root = jnp.dot(factor, inverse_root, precision=lax.Precision.HIGHEST)
    forcing_term = jnp.dot(scaled, rooted * innovation, precision=lax.Precision.HIGHEST) / spread
    inner_shift = jnp.dot(inverse_root, forcing_term, precision=lax.Precision.HIGHEST)
    mean_shift = jnp.dot(inverse_root, inner_shift, precision=lax.Precision.HIGHEST) / norm_fro
    transform = inverse_root / jnp.sqrt(norm_fro) + mean_shift[:, None]
    updated = average[None, :] + jnp.dot(transform.T, anomaly, precision=lax.Precision.HIGHEST)
    return updated.astype(jnp.bfloat16)

def reference(state, adjacent_columns, adjacent_rates, amplification_speed, obs_patch, obs_row, obs_value, obs_error):
    model_variable_array = state
    for section_index in range(STEPS):
        model_variable_array = propagate_prediction(model_variable_array, adjacent_columns, adjacent_rates, amplification_speed)
    rounded = model_variable_array.astype(jnp.bfloat16)
    widened = lax.optimization_barrier(rounded).astype(jnp.float32)
    grouped = widened.reshape(MEMBERS, LEVELS, PATCHES, PATCH_CELLS).transpose(2, 0, 1, 3)
    grouped = grouped.reshape(PATCHES, MEMBERS, LEVELS * PATCH_CELLS)
    is_live = obs_patch >= 0
    sort_key = jnp.where(is_live, obs_patch, PATCHES).astype(jnp.int32)
    ordering = jnp.argsort(sort_key, stable=True)
    sorted_key = sort_key[ordering]
    starts = jnp.searchsorted(sorted_key, jnp.arange(PATCHES, dtype=jnp.int32)).astype(jnp.int32)
    ranking = jnp.arange(OBS_TOTAL, dtype=jnp.int32) - starts[jnp.minimum(sorted_key, PATCHES - 1)]
    row_grid = jnp.zeros((PATCHES, PATCH_OBS), jnp.int32).at[sorted_key, ranking].set(obs_row[ordering].astype(jnp.int32), mode='drop')
    value_grid = jnp.zeros((PATCHES, PATCH_OBS), jnp.float32).at[sorted_key, ranking].set(obs_value[ordering], mode='drop')
    weight_all = 1.0 / (obs_error * obs_error)
    analysis_coefficient_array = jnp.zeros((PATCHES, PATCH_OBS), jnp.float32).at[sorted_key, ranking].set(weight_all[ordering], mode='drop')
    analysed = lax.map(lambda bundle: analyse(bundle[0], bundle[1], bundle[2], bundle[3]), (grouped, row_grid, value_grid, analysis_coefficient_array))
    analysed = analysed.reshape(PATCHES, MEMBERS, LEVELS, PATCH_CELLS).transpose(1, 2, 0, 3)
    return analysed.reshape(MEMBERS, LEVELS, CELLS)
```

```python
import functools
import math

import jax
import jax.numpy as jnp
from jax import lax
from jax.experimental import pallas as pl
from jax.experimental.pallas import tpu as pltpu
from jax.sharding import PartitionSpec as P

PATCH_CELLS = 128
RIM = 256
STEPS = 3
NS_ITERS = 6
LEVELS = 8
BLOCK = 256
WINDOW = BLOCK + 2 * RIM
HALO = STEPS * RIM
COEF_ROWS = 16


def high(value):
    return value.astype(jnp.bfloat16)


def low(value):
    return (value - high(value).astype(jnp.float32)).astype(jnp.bfloat16)


def dot_f32(a, b, dims=(((1,), (0,)), ((), ()))):
    return lax.dot_general(a, b, dims, preferred_element_type=jnp.float32)


def dot_split(a, b, dims=(((1,), (0,)), ((), ()))):
    ah, al, bh, bl = high(a), low(a), high(b), low(b)
    return dot_f32(ah, bh, dims) + (dot_f32(ah, bl, dims) + dot_f32(al, bh, dims))


def build_matrix(matrix_ref, index, offsets, rates, rows=32):
    column = lax.broadcasted_iota(jnp.int32, (1, BLOCK), 1)
    local = [
        jnp.broadcast_to(offsets[k : k + 1] + RIM + column, (8, BLOCK)) for k in range(6)
    ]
    rate = [jnp.broadcast_to(rates[k : k + 1], (8, BLOCK)) for k in range(6)]

    def chunk(step, carry):
        base = step * rows
        parts = []
        for part in range(rows // 8):
            row = lax.broadcasted_iota(jnp.int32, (8, BLOCK), 0) + (base + part * 8)
            total = jnp.where(row == local[0], rate[0], 0.0)
            for k in range(1, 6):
                total = total + jnp.where(row == local[k], rate[k], 0.0)
            parts.append(total)
        block = jnp.concatenate(parts, axis=0).astype(jnp.bfloat16)
        matrix_ref[index, pl.ds(pl.multiple_of(base, rows), rows), :] = block
        return carry

    lax.fori_loop(0, WINDOW // rows, chunk, 0)


def forecast_kernel(
    state_ref, left_ref, right_ref, offset_ref, rate_ref, speed_ref, out_ref,
    matrix_ref, field_a, field_b, wide_ref,
):
    rows, cells = state_ref.shape
    own_blocks = cells // BLOCK
    side_blocks = (STEPS - 1) * RIM // BLOCK
    blocks = own_blocks + 2 * side_blocks
    keep, speed = [], []
    for b in range(blocks):
        if b < side_blocks or b >= side_blocks + own_blocks:
            ref = left_ref if b < side_blocks else right_ref
            start = RIM + b * BLOCK if b < side_blocks else (b - side_blocks - own_blocks) * BLOCK
            coef = ref[rows:, start : start + BLOCK].astype(jnp.float32)
            offsets = coef[0:6].astype(jnp.int32)
            rates = coef[6:12]
            total = coef[12:13] + coef[13:14]
            quick = coef[14:15] + coef[15:16]
        else:
            start = (b - side_blocks) * BLOCK
            offsets = offset_ref[:, start : start + BLOCK]
            rates = rate_ref[:, start : start + BLOCK]
            total = jnp.sum(rates, axis=0, keepdims=True)
            quick = speed_ref[:, start : start + BLOCK]
        build_matrix(matrix_ref, b, offsets, rates)
        keep.append(1.0 - total)
        speed.append(quick)
    field_a[:, :HALO] = left_ref[:rows]
    field_a[:, HALO : HALO + cells] = state_ref[...].astype(jnp.bfloat16)
    field_a[:, HALO + cells :] = right_ref[:rows]
    source, target = field_a, field_b
    for step in range(STEPS):
        for b in range(step, blocks - step):
            first = b * BLOCK
            middle = slice(first + RIM, first + RIM + BLOCK)
            summed = dot_f32(source[:, first : first + WINDOW], matrix_ref[b])
            if step > 0:
                centre = wide_ref[:, middle]
            elif side_blocks <= b < side_blocks + own_blocks:
                own = (b - side_blocks) * BLOCK
                centre = state_ref[:, own : own + BLOCK]
            else:
                centre = source[:, middle].astype(jnp.float32)
            blended = centre * keep[b] + summed
            result = blended + speed[b] * jnp.tanh(blended)
            if step < STEPS - 1:
                wide_ref[:, middle] = result
                target[:, middle] = result.astype(jnp.bfloat16)
            else:
                patch = (first + RIM - HALO) // PATCH_CELLS
                for half in range(BLOCK // PATCH_CELLS):
                    piece = result[:, half * PATCH_CELLS : (half + 1) * PATCH_CELLS]
                    out_ref[patch + half] = piece.astype(jnp.bfloat16)
        source, target = target, source


def forecast(state, left, right, offsets, rates, speed):
    rows, cells = state.shape
    blocks = (cells + 2 * (STEPS - 1) * RIM) // BLOCK
    padded = cells + 2 * HALO
    return pl.pallas_call(
        forecast_kernel,
        out_shape=jax.ShapeDtypeStruct((cells // PATCH_CELLS, rows, PATCH_CELLS), jnp.bfloat16),
        in_specs=[pl.BlockSpec(memory_space=pltpu.VMEM)] * 6,
        out_specs=pl.BlockSpec(memory_space=pltpu.VMEM),
        scratch_shapes=[
            pltpu.VMEM((blocks, WINDOW, BLOCK), jnp.bfloat16),
            pltpu.VMEM((rows, padded), jnp.bfloat16),
            pltpu.VMEM((rows, padded), jnp.bfloat16),
            pltpu.VMEM((rows, padded), jnp.float32),
        ],
        name="forecast",
    )(state, left, right, offsets, rates, speed)


def analysis_kernel(x_ref, message_ref, out_ref, wide_ref, x2_ref, select_ref):
    members = x_ref.shape[0] // LEVELS
    span = LEVELS * PATCH_CELLS
    wide_ref[...] = x_ref[...].astype(jnp.float32)
    for level in range(LEVELS):
        part = wide_ref[pl.ds(level, members, stride=LEVELS), :]
        x2_ref[:, level * PATCH_CELLS : (level + 1) * PATCH_CELLS] = part.astype(jnp.bfloat16)
    location = jnp.concatenate([message_ref[0:1], message_ref[3:4]], axis=1) - 1.0
    value = jnp.concatenate([message_ref[1:2], message_ref[4:5]], axis=1)
    weight = jnp.concatenate([message_ref[2:3], message_ref[5:6]], axis=1)
    slots = location.shape[1]
    location = location.astype(jnp.int32)
    for first in range(0, span, PATCH_CELLS):
        row = lax.broadcasted_iota(jnp.int32, (PATCH_CELLS, slots), 0) + first
        hot = jnp.where(row == location, 1.0, 0.0)
        select_ref[first : first + PATCH_CELLS, :] = hot.astype(jnp.bfloat16)
    seen = dot_f32(x2_ref[...], select_ref[...])
    seen_mean = jnp.sum(seen, axis=0, keepdims=True) * (1.0 / members)
    rooted = jnp.sqrt(weight)
    spread = 1.0 / math.sqrt(members - 1.0)
    scaled = (seen - seen_mean) * (rooted * spread)
    row = lax.broadcasted_iota(jnp.int32, (members, members), 0)
    column = lax.broadcasted_iota(jnp.int32, (members, members), 1)
    diagonal = jnp.where(row == column, 1.0, 0.0)
    system = diagonal + dot_split(scaled, scaled, (((1,), (1,)), ((), ())))
    square = jnp.sum(jnp.sum(system * system, axis=0, keepdims=True), axis=1, keepdims=True)
    inverse_scale = lax.rsqrt(square)
    innovation = rooted * (value - seen_mean) * spread
    forcing = jnp.sum(scaled * innovation, axis=1, keepdims=True)
    iterate = system * inverse_scale
    factor = 1.5 * diagonal - 0.5 * iterate
    inverse_root = factor
    iterate = dot_split(iterate, factor)
    for sweep in range(1, NS_ITERS):
        factor = 1.5 * diagonal - 0.5 * dot_split(inverse_root, iterate)
        if sweep < NS_ITERS - 1:
            iterate = dot_split(iterate, factor)
        inverse_root = dot_split(factor, inverse_root)
    inner = jnp.sum(inverse_root * forcing, axis=0, keepdims=True)
    shift = jnp.sum(inverse_root * inner, axis=1, keepdims=True) * inverse_scale
    transform = (inverse_root * jnp.sqrt(inverse_scale)).astype(jnp.bfloat16)
    for level in range(LEVELS):
        part = x2_ref[:, level * PATCH_CELLS : (level + 1) * PATCH_CELLS].astype(jnp.float32)
        mean = jnp.sum(part, axis=0, keepdims=True) * (1.0 / members)
        anomaly = part - mean
        moved = mean + jnp.sum(anomaly * shift, axis=0, keepdims=True)
        updated = moved + dot_f32(transform, anomaly.astype(jnp.bfloat16), (((0,), (0,)), ((), ())))
        wide_ref[pl.ds(level, members, stride=LEVELS), :] = updated
    out_ref[...] = wide_ref[...].astype(jnp.bfloat16)


def analysis(x, message):
    rows = x.shape[0]
    members = rows // LEVELS
    slots = 2 * message.shape[1]
    return pl.pallas_call(
        analysis_kernel,
        out_shape=jax.ShapeDtypeStruct(x.shape, jnp.bfloat16),
        in_specs=[pl.BlockSpec(memory_space=pltpu.VMEM)] * 2,
        out_specs=pl.BlockSpec(memory_space=pltpu.VMEM),
        scratch_shapes=[
            pltpu.VMEM((rows, PATCH_CELLS), jnp.float32),
            pltpu.VMEM((members, LEVELS * PATCH_CELLS), jnp.bfloat16),
            pltpu.VMEM((LEVELS * PATCH_CELLS, slots), jnp.bfloat16),
        ],
        name="analysis",
    )(x, message)


def observation_message(groups, regions, obs_patch, obs_row, obs_value, obs_error):
    devices = groups * regions
    target = jnp.arange(devices, dtype=jnp.int32)
    wanted = target % regions * groups + target // regions
    before = jnp.arange(obs_patch.shape[0], dtype=jnp.int32)
    earlier = (obs_patch[:, None] == obs_patch[None, :]) & (before[:, None] < before[None, :])
    rank = jnp.sum(earlier.astype(jnp.int32), axis=0)
    hit = obs_patch[None, :] == wanted[:, None]
    fields = jnp.stack([(obs_row + 1).astype(jnp.float32), obs_value, 1.0 / (obs_error * obs_error)])
    parts = []
    for slot in range(2):
        chosen = (hit & (rank[None, :] == slot)).astype(jnp.float32)
        parts.append(
            lax.dot_general(
                chosen, fields, (((1,), (1,)), ((), ())), precision=lax.Precision.HIGHEST
            )
        )
    return jnp.concatenate(parts + [jnp.zeros((devices, 2), jnp.float32)], axis=1)


def on_device(
    state, adjacent_columns, adjacent_rates, amplification_speed,
    obs_patch, obs_row, obs_value, obs_error,
):
    members, levels, cells = state.shape
    regions = lax.axis_size("region")
    groups = lax.axis_size("member")
    total = cells * regions
    first = lax.axis_index("region") * cells
    cell_index = first + jnp.arange(cells, dtype=jnp.int32)
    offsets = (adjacent_columns - cell_index[None, :] + total // 2) % total - total // 2
    flat = state.reshape(members * levels, cells)
    rate_sum = jnp.sum(adjacent_rates, axis=0, keepdims=True)
    speed = amplification_speed[None, :]
    sides = []
    for part in (slice(cells - HALO, cells), slice(0, HALO)):
        sides.append(
            jnp.concatenate(
                [
                    flat[:, part].astype(jnp.bfloat16),
                    offsets[:, part].astype(jnp.bfloat16),
                    adjacent_rates[:, part].astype(jnp.bfloat16),
                    high(rate_sum[:, part]),
                    low(rate_sum[:, part]),
                    high(speed[:, part]),
                    low(speed[:, part]),
                ],
                axis=0,
            )
        )
    up = [(i, (i + 1) % regions) for i in range(regions)]
    left = lax.ppermute(sides[0], "region", up)
    right = lax.ppermute(sides[1], "region", [(j, i) for i, j in up])
    message = observation_message(groups, regions, obs_patch, obs_row, obs_value, obs_error)
    message = lax.all_to_all(message, ("member", "region"), 0, 0, tiled=True)
    rounded = forecast(flat, left, right, offsets, adjacent_rates, speed)
    patched = lax.all_to_all(rounded, "member", 0, 0, tiled=True)
    analysed = analysis(patched.reshape(-1, PATCH_CELLS), message.T)
    returned = analysed.reshape(groups, members * levels, PATCH_CELLS)
    back = lax.all_to_all(returned, "member", 0, 0, tiled=True)
    return back.transpose(1, 0, 2).reshape(members, levels, cells)


def solution(mesh):
    placed = (
        P("member", None, "region"),
        P(None, "region"),
        P(None, "region"),
        P("region"),
        P(("member", "region")),
        P(("member", "region")),
        P(("member", "region")),
        P(("member", "region")),
    )
    return jax.shard_map(
        on_device, mesh=mesh, in_specs=placed, out_specs=P("member", None, "region"), check_vma=False
    )
```

```python
import functools
import math

import jax
import jax.numpy as jnp
from jax import lax
from jax.experimental import pallas as pl
from jax.experimental.pallas import tpu as pltpu
from jax.sharding import PartitionSpec as P

PATCH_CELLS = 128
RIM = 256
STEPS = 3
NS_ITERS = 6
LEVELS = 8
BLOCK = 256
WINDOW = BLOCK + 2 * RIM
HALO = STEPS * RIM
COEF_ROWS = 16
TILE = 128


def high(value):
    return value.astype(jnp.bfloat16)


def low(value):
    return (value - high(value).astype(jnp.float32)).astype(jnp.bfloat16)


def dot_f32(a, b, dims=(((1,), (0,)), ((), ()))):
    return lax.dot_general(a, b, dims, preferred_element_type=jnp.float32)


def dot_split(a, b, dims=(((1,), (0,)), ((), ()))):
    ah, al, bh, bl = high(a), low(a), high(b), low(b)
    return dot_f32(ah, bh, dims) + (dot_f32(ah, bl, dims) + dot_f32(al, bh, dims))


def cell_offsets(columns, first, total):
    cell = first + lax.broadcasted_iota(jnp.int32, columns.shape, 1)
    offset = columns - cell
    offset = jnp.where(offset > total // 2, offset - total, offset)
    return jnp.where(offset < -(total // 2), offset + total, offset)


def build_matrix(matrix_ref, index, offsets, rates):
    zero = jnp.zeros((TILE, TILE), jnp.bfloat16)
    row = lax.broadcasted_iota(jnp.int32, (TILE, TILE), 0).astype(jnp.float32)
    row = row.astype(jnp.bfloat16)
    lane = lax.broadcasted_iota(jnp.int32, (1, TILE), 1).astype(jnp.float32)
    reach = (TILE + 2 * RIM) // TILE
    for part in range(BLOCK // TILE):
        lanes = slice(part * TILE, (part + 1) * TILE)
        local = offsets[:, lanes] + (lane + float(RIM))
        rate = [
            jnp.broadcast_to(rates[k : k + 1, lanes].astype(jnp.bfloat16), (TILE, TILE))
            for k in range(6)
        ]
        for tile in range(WINDOW // TILE):
            rows = slice(tile * TILE, (tile + 1) * TILE)
            step = tile - part
            if step < 0 or step >= reach:
                matrix_ref[index, rows, lanes] = zero
                continue
            total = None
            for k in range(6):
                near = (local[k : k + 1] - float(step * TILE)).astype(jnp.bfloat16)
                hit = row == jnp.broadcast_to(near, (TILE, TILE))
                term = jnp.where(hit, rate[k], zero)
                total = term if total is None else total + term
            matrix_ref[index, rows, lanes] = total


def prepare_kernel(first_ref, state_ref, column_ref, rate_ref, speed_ref, up_ref, down_ref, *, total):
    rows, cells = state_ref.shape
    offsets = cell_offsets(column_ref[...], first_ref[0], total).astype(jnp.float32)
    rates = rate_ref[...]
    rate_sum = jnp.sum(rates, axis=0, keepdims=True)
    speed = speed_ref[...]
    coef = jnp.concatenate(
        [
            offsets,
            rates,
            high(rate_sum).astype(jnp.float32),
            low(rate_sum).astype(jnp.float32),
            high(speed).astype(jnp.float32),
            low(speed).astype(jnp.float32),
        ],
        axis=0,
    ).astype(jnp.bfloat16)
    for ref, begin in ((up_ref, cells - HALO), (down_ref, 0)):
        ref[:rows] = state_ref[:, begin : begin + HALO].astype(jnp.bfloat16)
        ref[rows:] = coef[:, begin : begin + HALO]


def vmem(count):
    return [pl.BlockSpec(memory_space=pltpu.VMEM)] * count


def prepare(first, state, columns, rates, speed, total):
    rows, cells = state.shape
    side = jax.ShapeDtypeStruct((rows + COEF_ROWS, HALO), jnp.bfloat16)
    return pl.pallas_call(
        functools.partial(prepare_kernel, total=total),
        out_shape=(side, side),
        in_specs=[pl.BlockSpec(memory_space=pltpu.SMEM)] + vmem(4),
        out_specs=tuple(vmem(2)),
        compiler_params=pltpu.CompilerParams(vmem_limit_bytes=8 << 20),
        name="prepare",
    )(first, state, columns, rates, speed)


def local_kernel(
    first_ref, column_ref, rate_ref, patch_ref, row_ref, value_ref, error_ref,
    matrix_ref, message_ref, *, total, regions, groups,
):
    cells = column_ref.shape[1]
    offsets = cell_offsets(column_ref[...], first_ref[0], total).astype(jnp.float32)
    rates = rate_ref[...]
    for b in range(cells // BLOCK):
        part = slice(b * BLOCK, (b + 1) * BLOCK)
        build_matrix(matrix_ref, b, offsets[:, part], rates[:, part])
    devices, count = message_ref.shape[0], patch_ref.shape[1]
    target = lax.broadcasted_iota(jnp.int32, (devices, count), 0)
    wanted = target % regions * groups + target // regions
    hit = jnp.where(patch_ref[...] == wanted, 1.0, 0.0)
    before = lax.broadcasted_iota(jnp.int32, (count, count), 0)
    after = lax.broadcasted_iota(jnp.int32, (count, count), 1)
    earlier = jnp.where(before < after, 1.0, 0.0).astype(jnp.bfloat16)
    rank = dot_f32(hit.astype(jnp.bfloat16), earlier)
    field = lax.broadcasted_iota(jnp.int32, (message_ref.shape[1], count), 0)
    location = row_ref[...].astype(jnp.float32) + 1.0
    weight = 1.0 / (error_ref[...] * error_ref[...])
    message = None
    for slot in range(2):
        chosen = jnp.where(rank == float(slot), hit, 0.0).astype(jnp.bfloat16)
        values = jnp.zeros(field.shape, jnp.float32)
        for k, item in enumerate((location, value_ref[...], weight)):
            values = jnp.where(field == 3 * slot + k, item, values)
        for _ in range(3):
            piece = high(values)
            values = values - piece.astype(jnp.float32)
            term = dot_f32(chosen, piece, (((1,), (1,)), ((), ())))
            message = term if message is None else message + term
    message_ref[...] = message


def local_work(first, columns, rates, patch, row, value, error, total, regions, groups):
    cells = columns.shape[1]
    return pl.pallas_call(
        functools.partial(local_kernel, total=total, regions=regions, groups=groups),
        out_shape=(
            jax.ShapeDtypeStruct((cells // BLOCK, WINDOW, BLOCK), jnp.bfloat16),
            jax.ShapeDtypeStruct((regions * groups, TILE), jnp.float32),
        ),
        in_specs=[pl.BlockSpec(memory_space=pltpu.SMEM)] + vmem(6),
        out_specs=tuple(vmem(2)),
        compiler_params=pltpu.CompilerParams(vmem_limit_bytes=8 << 20),
        name="local_work",
    )(first, columns, rates, patch, row, value, error)


def forecast_kernel(
    state_ref, left_ref, right_ref, own_ref, rate_ref, speed_ref, out_ref,
    matrix_ref, field_a, field_b, wide_ref,
):
    rows, cells = state_ref.shape
    own_blocks = cells // BLOCK
    side_blocks = (STEPS - 1) * RIM // BLOCK
    blocks = own_blocks + 2 * side_blocks
    keep, speed, matrices = [], [], []
    for b in range(blocks):
        if b < side_blocks or b >= side_blocks + own_blocks:
            ref = left_ref if b < side_blocks else right_ref
            start = RIM + b * BLOCK if b < side_blocks else (b - side_blocks - own_blocks) * BLOCK
            index = b if b < side_blocks else b - own_blocks
            coef = ref[rows:, start : start + BLOCK].astype(jnp.float32)
            build_matrix(matrix_ref, index, coef[0:6], coef[6:12])
            total = coef[12:13] + coef[13:14]
            quick = coef[14:15] + coef[15:16]
            matrices.append((matrix_ref, index))
        else:
            start = (b - side_blocks) * BLOCK
            total = jnp.sum(rate_ref[:, start : start + BLOCK], axis=0, keepdims=True)
            quick = speed_ref[:, start : start + BLOCK]
            matrices.append((own_ref, b - side_blocks))
        keep.append(1.0 - total)
        speed.append(quick)
    field_a[:, :HALO] = left_ref[:rows]
    field_a[:, HALO : HALO + cells] = state_ref[...].astype(jnp.bfloat16)
    field_a[:, HALO + cells :] = right_ref[:rows]
    source, target = field_a, field_b
    for step in range(STEPS):
        for b in range(step, blocks - step):
            first = b * BLOCK
            middle = slice(first + RIM, first + RIM + BLOCK)
            holder, index = matrices[b]
            summed = dot_f32(source[:, first : first + WINDOW], holder[index])
            if step > 0:
                centre = wide_ref[:, middle]
            elif side_blocks <= b < side_blocks + own_blocks:
                own = (b - side_blocks) * BLOCK
                centre = state_ref[:, own : own + BLOCK]
            else:
                centre = source[:, middle].astype(jnp.float32)
            blended = centre * keep[b] + summed
            result = blended + speed[b] * jnp.tanh(blended)
            if step < STEPS - 1:
                wide_ref[:, middle] = result
                target[:, middle] = result.astype(jnp.bfloat16)
            else:
                patch = (first + RIM - HALO) // PATCH_CELLS
                for half in range(BLOCK // PATCH_CELLS):
                    piece = result[:, half * PATCH_CELLS : (half + 1) * PATCH_CELLS]
                    out_ref[patch + half] = piece.astype(jnp.bfloat16)
        source, target = target, source


def forecast(state, left, right, own, rates, speed):
    rows, cells = state.shape
    sides = 2 * (STEPS - 1) * RIM // BLOCK
    padded = cells + 2 * HALO
    return pl.pallas_call(
        forecast_kernel,
        out_shape=jax.ShapeDtypeStruct((cells // PATCH_CELLS, rows, PATCH_CELLS), jnp.bfloat16),
        in_specs=vmem(6),
        out_specs=pl.BlockSpec(memory_space=pltpu.VMEM),
        scratch_shapes=[
            pltpu.VMEM((sides, WINDOW, BLOCK), jnp.bfloat16),
            pltpu.VMEM((rows, padded), jnp.bfloat16),
            pltpu.VMEM((rows, padded), jnp.bfloat16),
            pltpu.VMEM((rows, padded), jnp.float32),
        ],
        compiler_params=pltpu.CompilerParams(vmem_limit_bytes=20 << 20),
        name="forecast",
    )(state, left, right, own, rates, speed)


def analysis_kernel(x_ref, message_ref, out_ref, wide_ref, x2_ref, select_ref):
    members = x_ref.shape[0] // LEVELS
    span = LEVELS * PATCH_CELLS
    wide_ref[...] = x_ref[...].astype(jnp.float32)
    for level in range(LEVELS):
        part = wide_ref[pl.ds(level, members, stride=LEVELS), :]
        x2_ref[:, level * PATCH_CELLS : (level + 1) * PATCH_CELLS] = part.astype(jnp.bfloat16)
    message = jnp.transpose(message_ref[...])
    location = jnp.concatenate([message[0:1], message[3:4]], axis=1) - 1.0
    value = jnp.concatenate([message[1:2], message[4:5]], axis=1)
    weight = jnp.concatenate([message[2:3], message[5:6]], axis=1)
    slots = location.shape[1]
    location = location.astype(jnp.int32)
    for first in range(0, span, PATCH_CELLS):
        row = lax.broadcasted_iota(jnp.int32, (PATCH_CELLS, slots), 0) + first
        hot = jnp.where(row == location, 1.0, 0.0)
        select_ref[first : first + PATCH_CELLS, :] = hot.astype(jnp.bfloat16)
    seen = dot_f32(x2_ref[...], select_ref[...])
    seen_mean = jnp.sum(seen, axis=0, keepdims=True) * (1.0 / members)
    rooted = jnp.sqrt(weight)
    spread = 1.0 / math.sqrt(members - 1.0)
    scaled = (seen - seen_mean) * (rooted * spread)
    row = lax.broadcasted_iota(jnp.int32, (members, members), 0)
    column = lax.broadcasted_iota(jnp.int32, (members, members), 1)
    diagonal = jnp.where(row == column, 1.0, 0.0)
    system = diagonal + dot_split(scaled, scaled, (((1,), (1,)), ((), ())))
    square = jnp.sum(jnp.sum(system * system, axis=0, keepdims=True), axis=1, keepdims=True)
    inverse_scale = lax.rsqrt(square)
    innovation = rooted * (value - seen_mean) * spread
    forcing = jnp.sum(scaled * innovation, axis=1, keepdims=True)
    iterate = system * inverse_scale
    factor = 1.5 * diagonal - 0.5 * iterate
    inverse_root = factor
    iterate = dot_split(iterate, factor)
    for sweep in range(1, NS_ITERS):
        factor = 1.5 * diagonal - 0.5 * dot_split(inverse_root, iterate)
        if sweep < NS_ITERS - 1:
            iterate = dot_split(iterate, factor)
        inverse_root = dot_split(factor, inverse_root)
    inner = jnp.sum(inverse_root * forcing, axis=0, keepdims=True)
    shift = jnp.sum(inverse_root * inner, axis=1, keepdims=True) * inverse_scale
    transform = (inverse_root * jnp.sqrt(inverse_scale)).astype(jnp.bfloat16)
    for level in range(LEVELS):
        part = x2_ref[:, level * PATCH_CELLS : (level + 1) * PATCH_CELLS].astype(jnp.float32)
        mean = jnp.sum(part, axis=0, keepdims=True) * (1.0 / members)
        anomaly = part - mean
        moved = mean + jnp.sum(anomaly * shift, axis=0, keepdims=True)
        updated = moved + dot_f32(transform, anomaly.astype(jnp.bfloat16), (((0,), (0,)), ((), ())))
        wide_ref[pl.ds(level, members, stride=LEVELS), :] = updated
    out_ref[...] = wide_ref[...].astype(jnp.bfloat16)


def analysis(x, message):
    rows = x.shape[0]
    members = rows // LEVELS
    slots = 2 * message.shape[0]
    return pl.pallas_call(
        analysis_kernel,
        out_shape=jax.ShapeDtypeStruct(x.shape, jnp.bfloat16),
        in_specs=vmem(2),
        out_specs=pl.BlockSpec(memory_space=pltpu.VMEM),
        compiler_params=pltpu.CompilerParams(vmem_limit_bytes=12 << 20),
        scratch_shapes=[
            pltpu.VMEM((rows, PATCH_CELLS), jnp.float32),
            pltpu.VMEM((members, LEVELS * PATCH_CELLS), jnp.bfloat16),
            pltpu.VMEM((LEVELS * PATCH_CELLS, slots), jnp.bfloat16),
        ],
        name="analysis",
    )(x, message)


def on_device(
    state, adjacent_columns, adjacent_rates, amplification_speed,
    obs_patch, obs_row, obs_value, obs_error,
):
    members, levels, cells = state.shape
    regions = lax.axis_size("region")
    groups = lax.axis_size("member")
    total = cells * regions
    first = (lax.axis_index("region") * cells).astype(jnp.int32).reshape(1)
    flat = state.reshape(members * levels, cells)
    speed = amplification_speed[None, :]
    sides = prepare(first, flat, adjacent_columns, adjacent_rates, speed, total)
    up = [(i, (i + 1) % regions) for i in range(regions)]
    left = lax.ppermute(sides[0], "region", up)
    right = lax.ppermute(sides[1], "region", [(j, i) for i, j in up])
    own, message = local_work(
        first, adjacent_columns, adjacent_rates, obs_patch[None, :], obs_row[None, :],
        obs_value[None, :], obs_error[None, :], total, regions, groups,
    )
    message = lax.all_to_all(message, ("member", "region"), 0, 0, tiled=True)
    rounded = forecast(flat, left, right, own, adjacent_rates, speed)
    patched = lax.all_to_all(rounded, "member", 0, 0, tiled=True)
    analysed = analysis(patched.reshape(-1, PATCH_CELLS), message)
    returned = analysed.reshape(groups, members * levels, PATCH_CELLS)
    back = lax.all_to_all(returned, "member", 0, 0, tiled=True)
    back = back.reshape(groups, members, levels, PATCH_CELLS)
    return back.transpose(1, 2, 0, 3).reshape(members, levels, cells)


def solution(mesh):
    placed = (
        P("member", None, "region"),
        P(None, "region"),
        P(None, "region"),
        P("region"),
        P(("member", "region")),
        P(("member", "region")),
        P(("member", "region")),
        P(("member", "region")),
    )
    return jax.shard_map(
        on_device, mesh=mesh, in_specs=placed, out_specs=P("member", None, "region"), check_vma=False
    )
```

```python
import functools
import math

import jax
import jax.numpy as jnp
from jax import lax
from jax.experimental import pallas as pl
from jax.experimental.pallas import tpu as pltpu
from jax.sharding import PartitionSpec as P

PATCH_CELLS = 128
RIM = 256
STEPS = 3
NS_ITERS = 6
LEVELS = 8
BLOCK = 256
WINDOW = BLOCK + 2 * RIM
HALO = STEPS * RIM
COEF_ROWS = 16
TILE = 128
STATE_CHUNKS = 4


def high(value):
    return value.astype(jnp.bfloat16)


def low(value):
    return (value - high(value).astype(jnp.float32)).astype(jnp.bfloat16)


def dot_f32(a, b, dims=(((1,), (0,)), ((), ()))):
    return lax.dot_general(a, b, dims, preferred_element_type=jnp.float32)


def dot_half(a, b, dims=(((1,), (0,)), ((), ()))):
    return dot_f32(high(a), high(b), dims)


def cell_offsets(columns, first, total):
    cell = first + lax.broadcasted_iota(jnp.int32, columns.shape, 1)
    offset = columns - cell
    offset = jnp.where(offset > total // 2, offset - total, offset)
    return jnp.where(offset < -(total // 2), offset + total, offset)


def build_matrix(matrix_ref, index, offsets, rates):
    zero = jnp.zeros((TILE, TILE), jnp.bfloat16)
    row = lax.broadcasted_iota(jnp.int32, (TILE, TILE), 0).astype(jnp.float32)
    row = row.astype(jnp.bfloat16)
    lane = lax.broadcasted_iota(jnp.int32, (1, TILE), 1).astype(jnp.float32)
    reach = (TILE + 2 * RIM) // TILE
    for part in range(BLOCK // TILE):
        lanes = slice(part * TILE, (part + 1) * TILE)
        local = offsets[:, lanes] + (lane + float(RIM))
        rate = [
            jnp.broadcast_to(rates[k : k + 1, lanes].astype(jnp.bfloat16), (TILE, TILE))
            for k in range(6)
        ]
        for tile in range(WINDOW // TILE):
            rows = slice(tile * TILE, (tile + 1) * TILE)
            step = tile - part
            if step < 0 or step >= reach:
                matrix_ref[index, rows, lanes] = zero
                continue
            total = None
            for k in range(6):
                near = (local[k : k + 1] - float(step * TILE)).astype(jnp.bfloat16)
                hit = row == jnp.broadcast_to(near, (TILE, TILE))
                term = jnp.where(hit, rate[k], zero)
                total = term if total is None else total + term
            matrix_ref[index, rows, lanes] = total


def prepare_kernel(
    state_hbm, column_hbm, rate_hbm, speed_hbm, patch_hbm, row_hbm, value_hbm, error_hbm,
    wide_pair_ref, near_pair_ref, state_ref, coef_ref, message_ref,
    column_ref, rate_ref, speed_ref, patch_ref, row_ref, value_ref, error_ref, small_sem, state_sem,
    *, total, regions, groups,
):
    rows, cells = state_ref.shape
    small = [
        pltpu.make_async_copy(source, target, small_sem.at[i])
        for i, (source, target) in enumerate(
            (
                (column_hbm, column_ref),
                (rate_hbm, rate_ref),
                (speed_hbm, speed_ref),
                (patch_hbm, patch_ref),
                (row_hbm, row_ref),
                (value_hbm, value_ref),
                (error_hbm, error_ref),
            )
        )
    ]
    chunk = rows // STATE_CHUNKS
    large = [
        pltpu.make_async_copy(
            state_hbm.at[pl.ds(i * chunk, chunk)],
            state_ref.at[pl.ds(i * chunk, chunk)],
            state_sem.at[i],
        )
        for i in range(STATE_CHUNKS)
    ]
    for copy in small + large:
        copy.start()
    for copy in small:
        copy.wait()
    region = lax.axis_index("region")
    odd = region % 2
    last = cells - HALO
    wide_first = pl.multiple_of(odd * last, TILE)
    near_first = pl.multiple_of((1 - odd) * last, TILE)
    offsets = cell_offsets(column_ref[...], region * cells, total).astype(jnp.float32)
    rates = rate_ref[...]
    rate_sum = jnp.sum(rates, axis=0, keepdims=True)
    speed = speed_ref[...]
    coef_ref[...] = jnp.concatenate(
        [
            offsets,
            rates,
            high(rate_sum).astype(jnp.float32),
            low(rate_sum).astype(jnp.float32),
            high(speed).astype(jnp.float32),
            low(speed).astype(jnp.float32),
        ],
        axis=0,
    )
    wide_pair_ref[rows:] = coef_ref[:, pl.ds(wide_first, HALO)].astype(jnp.bfloat16)
    near_pair_ref[rows:] = coef_ref[:, pl.ds(near_first, HALO)].astype(jnp.bfloat16)
    devices, count = message_ref.shape[0], patch_ref.shape[1]
    target = lax.broadcasted_iota(jnp.int32, (devices, count), 0)
    wanted = target % regions * groups + target // regions
    hit = jnp.where(patch_ref[...] == wanted, 1.0, 0.0)
    before = lax.broadcasted_iota(jnp.int32, (count, count), 0)
    after = lax.broadcasted_iota(jnp.int32, (count, count), 1)
    earlier = jnp.where(before < after, 1.0, 0.0).astype(jnp.bfloat16)
    rank = dot_f32(hit.astype(jnp.bfloat16), earlier)
    field = lax.broadcasted_iota(jnp.int32, (message_ref.shape[1], count), 0)
    location = row_ref[...].astype(jnp.float32) + 1.0
    weight = 1.0 / (error_ref[...] * error_ref[...])
    message = None
    for slot in range(2):
        chosen = jnp.where(rank == float(slot), hit, 0.0).astype(jnp.bfloat16)
        values = jnp.zeros(field.shape, jnp.float32)
        for k, item in enumerate((location, value_ref[...], weight)):
            values = jnp.where(field == 3 * slot + k, item, values)
        for _ in range(3):
            piece = high(values)
            values = values - piece.astype(jnp.float32)
            term = dot_f32(chosen, piece, (((1,), (1,)), ((), ())))
            message = term if message is None else message + term
    message_ref[...] = message
    for i, copy in enumerate(large):
        copy.wait()
        part = pl.ds(i * chunk, chunk)
        wide_pair_ref[part] = state_ref[part, pl.ds(wide_first, HALO)].astype(jnp.bfloat16)
        near_pair_ref[part] = state_ref[part, pl.ds(near_first, HALO)].astype(jnp.bfloat16)


def vmem(count):
    return [pl.BlockSpec(memory_space=pltpu.VMEM)] * count


def in_vmem(*values):
    return [pltpu.with_memory_space_constraint(value, pltpu.VMEM) for value in values]


def in_hbm(*values):
    return [pltpu.with_memory_space_constraint(value, pltpu.HBM) for value in values]


def prepare(state, columns, rates, speed, patch, row, value, error, total, regions, groups):
    rows, cells = state.shape
    count = patch.shape[1]
    side = pltpu.VMEM((rows + COEF_ROWS, HALO), jnp.bfloat16)
    return pl.pallas_call(
        functools.partial(prepare_kernel, total=total, regions=regions, groups=groups),
        out_shape=(
            side,
            side,
            pltpu.VMEM((rows, cells), jnp.float32),
            pltpu.VMEM((COEF_ROWS, cells), jnp.float32),
            jax.ShapeDtypeStruct((regions * groups, TILE), jnp.float32),
        ),
        in_specs=[pl.BlockSpec(memory_space=pltpu.HBM)] * 8,
        out_specs=tuple(vmem(5)),
        scratch_shapes=[
            pltpu.VMEM(columns.shape, jnp.int32),
            pltpu.VMEM(rates.shape, jnp.float32),
            pltpu.VMEM(speed.shape, jnp.float32),
            pltpu.VMEM((1, count), jnp.int32),
            pltpu.VMEM((1, count), jnp.int32),
            pltpu.VMEM((1, count), jnp.float32),
            pltpu.VMEM((1, count), jnp.float32),
            pltpu.SemaphoreType.DMA((7,)),
            pltpu.SemaphoreType.DMA((STATE_CHUNKS,)),
        ],
        compiler_params=pltpu.CompilerParams(vmem_limit_bytes=8 << 20),
        name="prepare",
    )(*in_hbm(state, columns, rates, speed, patch, row, value, error))


def matrices_kernel(coef_ref, matrix_ref):
    for b in range(matrix_ref.shape[0]):
        part = slice(b * BLOCK, (b + 1) * BLOCK)
        build_matrix(matrix_ref, b, coef_ref[0:6, part], coef_ref[6:12, part])


def own_matrices(coef):
    shape = (coef.shape[1] // BLOCK, WINDOW, BLOCK)
    return pl.pallas_call(
        matrices_kernel,
        out_shape=pltpu.VMEM(shape, jnp.bfloat16),
        in_specs=vmem(1),
        out_specs=vmem(1)[0],
        compiler_params=pltpu.CompilerParams(vmem_limit_bytes=4 << 20),
        name="own_matrices",
    )(*in_vmem(coef))


def forecast_kernel(
    state_ref, wide_pair_ref, near_pair_ref, own_ref, own_coef_ref, out_ref,
    matrix_ref, coef_ref, field_a, field_b, wide_ref,
):
    rows, cells = state_ref.shape
    own_blocks = cells // BLOCK
    side_blocks = (STEPS - 1) * RIM // BLOCK
    blocks = own_blocks + 2 * side_blocks
    odd = lax.axis_index("region") % 2
    far = HALO + cells
    for ref, begin in ((wide_pair_ref, odd * far), (near_pair_ref, (1 - odd) * far)):
        begin = pl.multiple_of(begin, TILE)
        coef_ref[:, pl.ds(begin, HALO)] = ref[rows:].astype(jnp.float32)
        field_a[:, pl.ds(begin, HALO)] = ref[:rows]
    coef_ref[:, HALO:far] = own_coef_ref[...]
    field_a[:, HALO:far] = state_ref[...].astype(jnp.bfloat16)
    keep, speed, matrices = [], [], []
    for b in range(blocks):
        part = slice(RIM + b * BLOCK, RIM + (b + 1) * BLOCK)
        if side_blocks <= b < side_blocks + own_blocks:
            matrices.append((own_ref, b - side_blocks))
        else:
            index = b if b < side_blocks else b - own_blocks
            build_matrix(matrix_ref, index, coef_ref[0:6, part], coef_ref[6:12, part])
            matrices.append((matrix_ref, index))
        keep.append(1.0 - (coef_ref[12:13, part] + coef_ref[13:14, part]))
        speed.append(coef_ref[14:15, part] + coef_ref[15:16, part])
    source, target = field_a, field_b
    for step in range(STEPS):
        for b in range(step, blocks - step):
            first = b * BLOCK
            middle = slice(first + RIM, first + RIM + BLOCK)
            holder, index = matrices[b]
            summed = dot_f32(source[:, first : first + WINDOW], holder[index])
            if step > 0:
                centre = wide_ref[:, middle]
            elif side_blocks <= b < side_blocks + own_blocks:
                own = (b - side_blocks) * BLOCK
                centre = state_ref[:, own : own + BLOCK]
            else:
                centre = source[:, middle].astype(jnp.float32)
            blended = centre * keep[b] + summed
            result = blended + speed[b] * jnp.tanh(blended)
            if step < STEPS - 1:
                wide_ref[:, middle] = result
                target[:, middle] = result.astype(jnp.bfloat16)
            else:
                patch = (first + RIM - HALO) // PATCH_CELLS
                for half in range(BLOCK // PATCH_CELLS):
                    piece = result[:, half * PATCH_CELLS : (half + 1) * PATCH_CELLS]
                    out_ref[patch + half] = piece.astype(jnp.bfloat16)
        source, target = target, source


def forecast(state, wide_pair, near_pair, own, coef):
    rows, cells = state.shape
    sides = 2 * (STEPS - 1) * RIM // BLOCK
    padded = cells + 2 * HALO
    return pl.pallas_call(
        forecast_kernel,
        out_shape=pltpu.VMEM((cells // PATCH_CELLS, rows, PATCH_CELLS), jnp.bfloat16),
        in_specs=vmem(5),
        out_specs=pl.BlockSpec(memory_space=pltpu.VMEM),
        scratch_shapes=[
            pltpu.VMEM((sides, WINDOW, BLOCK), jnp.bfloat16),
            pltpu.VMEM((COEF_ROWS, padded), jnp.float32),
            pltpu.VMEM((rows, padded), jnp.bfloat16),
            pltpu.VMEM((rows, padded), jnp.bfloat16),
            pltpu.VMEM((rows, padded), jnp.float32),
        ],
        compiler_params=pltpu.CompilerParams(vmem_limit_bytes=16 << 20),
        name="forecast",
    )(*in_vmem(state, wide_pair, near_pair, own, coef))


def analysis_kernel(x_ref, message_ref, out_ref, wide_ref, x2_ref, select_ref):
    members = x_ref.shape[0] // LEVELS
    span = LEVELS * PATCH_CELLS
    wide_ref[...] = x_ref[...].astype(jnp.float32)
    for level in range(LEVELS):
        part = wide_ref[pl.ds(level, members, stride=LEVELS), :]
        x2_ref[:, level * PATCH_CELLS : (level + 1) * PATCH_CELLS] = part.astype(jnp.bfloat16)
    message = jnp.transpose(message_ref[...])
    location = jnp.concatenate([message[0:1], message[3:4]], axis=1) - 1.0
    value = jnp.concatenate([message[1:2], message[4:5]], axis=1)
    weight = jnp.concatenate([message[2:3], message[5:6]], axis=1)
    slots = location.shape[1]
    location = location.astype(jnp.int32)
    for first in range(0, span, PATCH_CELLS):
        row = lax.broadcasted_iota(jnp.int32, (PATCH_CELLS, slots), 0) + first
        hot = jnp.where(row == location, 1.0, 0.0)
        select_ref[first : first + PATCH_CELLS, :] = hot.astype(jnp.bfloat16)
    seen = dot_f32(x2_ref[...], select_ref[...])
    seen_mean = jnp.sum(seen, axis=0, keepdims=True) * (1.0 / members)
    rooted = jnp.sqrt(weight)
    spread = 1.0 / math.sqrt(members - 1.0)
    scaled = (seen - seen_mean) * (rooted * spread)
    row = lax.broadcasted_iota(jnp.int32, (members, members), 0)
    column = lax.broadcasted_iota(jnp.int32, (members, members), 1)
    diagonal = jnp.where(row == column, 1.0, 0.0)
    product = dot_half(scaled, scaled, (((1,), (1,)), ((), ())))
    system = diagonal + product
    square = jnp.sum(jnp.sum(system * system, axis=0, keepdims=True), axis=1, keepdims=True)
    inverse_scale = jnp.broadcast_to(lax.rsqrt(square), (1, members))
    innovation = rooted * (value - seen_mean) * spread
    forcing = jnp.sum(scaled * innovation, axis=1, keepdims=True)
    p, z = inverse_scale, jnp.ones_like(inverse_scale)
    both = product * inverse_scale
    root = None
    for sweep in range(NS_ITERS):
        f = 1.5 - 0.5 * p
        factor = -0.5 * both
        narrow = factor.astype(jnp.bfloat16)
        if root is None:
            new_root = factor
        else:
            new_root = z * factor + f * root + dot_f32(high(root), narrow)
        if sweep < NS_ITERS - 1:
            once = p * factor + f * both + dot_f32(high(both), narrow)
            q = p * f
            both = q * factor + f * once + dot_f32(high(once), narrow)
            p = q * f
        root, z = new_root, z * f
    whole = root + z * diagonal
    inner = jnp.sum(whole * forcing, axis=0, keepdims=True)
    shift = jnp.sum(whole * inner, axis=1, keepdims=True) * inverse_scale[:, 0:1]
    half_scale = jnp.sqrt(inverse_scale)
    transform = (root * half_scale).astype(jnp.bfloat16)
    direct = (z * half_scale)[:, 0:PATCH_CELLS]
    pair = 2
    for level in range(0, LEVELS, pair):
        pieces = []
        for k in range(level, level + pair):
            part = x2_ref[:, k * PATCH_CELLS : (k + 1) * PATCH_CELLS].astype(jnp.float32)
            mean = jnp.sum(part, axis=0, keepdims=True) * (1.0 / members)
            anomaly = part - mean
            base = mean + jnp.sum(anomaly * shift, axis=0, keepdims=True) + direct * anomaly
            pieces.append((anomaly.astype(jnp.bfloat16), base))
        moved = dot_f32(transform, jnp.concatenate([piece[0] for piece in pieces], axis=1))
        for k in range(pair):
            updated = pieces[k][1] + moved[:, k * PATCH_CELLS : (k + 1) * PATCH_CELLS]
            wide_ref[pl.ds(level + k, members, stride=LEVELS), :] = updated
    out_ref[...] = wide_ref[...].astype(jnp.bfloat16)


def analysis(x, message):
    rows = x.shape[0]
    members = rows // LEVELS
    slots = 2 * message.shape[0]
    return pl.pallas_call(
        analysis_kernel,
        out_shape=pltpu.VMEM(x.shape, jnp.bfloat16),
        in_specs=vmem(2),
        out_specs=pl.BlockSpec(memory_space=pltpu.VMEM),
        compiler_params=pltpu.CompilerParams(vmem_limit_bytes=12 << 20),
        scratch_shapes=[
            pltpu.VMEM((rows, PATCH_CELLS), jnp.float32),
            pltpu.VMEM((members, LEVELS * PATCH_CELLS), jnp.bfloat16),
            pltpu.VMEM((LEVELS * PATCH_CELLS, slots), jnp.bfloat16),
        ],
        name="analysis",
    )(*in_vmem(x, message))


def on_device(
    state, adjacent_columns, adjacent_rates, amplification_speed,
    obs_patch, obs_row, obs_value, obs_error,
):
    members, levels, cells = state.shape
    regions = lax.axis_size("region")
    groups = lax.axis_size("member")
    total = cells * regions
    flat = state.reshape(members * levels, cells)
    wide_pair, near_pair, kept, coef, message = prepare(
        flat, adjacent_columns, adjacent_rates, amplification_speed[None, :],
        obs_patch[None, :], obs_row[None, :], obs_value[None, :], obs_error[None, :],
        total, regions, groups,
    )
    pairs = [(i, (i + 1) % regions) for i in range(regions)]
    wide_swap = [edge for i, j in pairs[1::2] for edge in ((i, j), (j, i))]
    near_swap = [edge for i, j in pairs[0::2] for edge in ((i, j), (j, i))]
    wide_pair = lax.ppermute(wide_pair, "region", wide_swap)
    near_pair = lax.ppermute(near_pair, "region", near_swap)
    message = lax.all_to_all(message, ("member", "region"), 0, 0, tiled=True)
    own = own_matrices(coef)
    rounded = forecast(kept, wide_pair, near_pair, own, coef)
    patched = lax.all_to_all(rounded, "member", 0, 0, tiled=True)
    analysed = analysis(patched.reshape(-1, PATCH_CELLS), message)
    returned = analysed.reshape(groups, members * levels, PATCH_CELLS)
    back = lax.all_to_all(returned, "member", 0, 0, tiled=True)
    back = back.reshape(groups, members, levels, PATCH_CELLS)
    return back.transpose(1, 2, 0, 3).reshape(members, levels, cells)


def solution(mesh):
    placed = (
        P("member", None, "region"),
        P(None, "region"),
        P(None, "region"),
        P("region"),
        P(("member", "region")),
        P(("member", "region")),
        P(("member", "region")),
        P(("member", "region")),
    )
    return jax.shard_map(
        on_device, mesh=mesh, in_specs=placed, out_specs=P("member", None, "region"), check_vma=False
    )
```

```python
import functools
import math

import jax
import jax.numpy as jnp
from jax import lax
from jax.experimental import pallas as pl
from jax.experimental.pallas import tpu as pltpu
from jax.sharding import PartitionSpec as P


PATCH_CELLS = 128
RIM = 256
STEPS = 3
NS_ITERS = 6
LEVELS = 8
BLOCK = 256
WINDOW = BLOCK + 2 * RIM
HALO = STEPS * RIM
COEF_ROWS = 16
TILE = 128
STATE_CHUNKS = 4
SHIFTS = 4


def high(value):
    return value.astype(jnp.bfloat16)


def low(value):
    return (value - high(value).astype(jnp.float32)).astype(jnp.bfloat16)


def dot_f32(a, b, dims=(((1,), (0,)), ((), ()))):
    return lax.dot_general(a, b, dims, preferred_element_type=jnp.float32)


def dot_half(a, b, dims=(((1,), (0,)), ((), ()))):
    return dot_f32(high(a), high(b), dims)


def cell_offsets(columns, first, total):
    cell = first + lax.broadcasted_iota(jnp.int32, columns.shape, 1)
    offset = columns - cell
    offset = jnp.where(offset > total // 2, offset - total, offset)
    return jnp.where(offset < -(total // 2), offset + total, offset)


def build_matrix(matrix_ref, index, offsets, rates):
    zero = jnp.zeros((TILE, TILE), jnp.bfloat16)
    row = lax.broadcasted_iota(jnp.int32, (TILE, TILE), 0).astype(jnp.float32)
    row = row.astype(jnp.bfloat16)
    lane = lax.broadcasted_iota(jnp.int32, (1, TILE), 1).astype(jnp.float32)
    reach = (TILE + 2 * RIM) // TILE
    for part in range(BLOCK // TILE):
        lanes = slice(part * TILE, (part + 1) * TILE)
        local = offsets[:, lanes] + (lane + float(RIM))
        rate = [
            jnp.broadcast_to(rates[k : k + 1, lanes].astype(jnp.bfloat16), (TILE, TILE))
            for k in range(6)
        ]
        for tile in range(WINDOW // TILE):
            rows = slice(tile * TILE, (tile + 1) * TILE)
            step = tile - part
            if step < 0 or step >= reach:
                matrix_ref[index, rows, lanes] = zero
                continue
            total = None
            for k in range(6):
                near = (local[k : k + 1] - float(step * TILE)).astype(jnp.bfloat16)
                hit = row == jnp.broadcast_to(near, (TILE, TILE))
                term = jnp.where(hit, rate[k], zero)
                total = term if total is None else total + term
            matrix_ref[index, rows, lanes] = total


def fetches(sources, targets, sem):
    return [
        pltpu.make_async_copy(source, target, sem.at[i])
        for i, (source, target) in enumerate(zip(sources, targets))
    ]


def prepare_kernel(
    state_hbm, column_hbm, rate_hbm, speed_hbm, wide_pair_ref, near_pair_ref, state_ref, coef_ref,
    column_ref, rate_ref, speed_ref, small_sem, state_sem, *, total,
):
    rows, cells = state_ref.shape
    small = fetches(
        (column_hbm, rate_hbm, speed_hbm), (column_ref, rate_ref, speed_ref), small_sem
    )
    chunk = rows // STATE_CHUNKS
    large = [
        pltpu.make_async_copy(
            state_hbm.at[pl.ds(i * chunk, chunk)],
            state_ref.at[pl.ds(i * chunk, chunk)],
            state_sem.at[i],
        )
        for i in range(STATE_CHUNKS)
    ]
    for copy in small + large:
        copy.start()
    for copy in small:
        copy.wait()
    region = lax.axis_index("region")
    odd = region % 2
    last = cells - HALO
    wide_first = pl.multiple_of(odd * last, TILE)
    near_first = pl.multiple_of((1 - odd) * last, TILE)
    offsets = cell_offsets(column_ref[...], region * cells, total).astype(jnp.float32)
    rates = rate_ref[...]
    rate_sum = jnp.sum(rates, axis=0, keepdims=True)
    speed = speed_ref[...]
    coef_ref[...] = jnp.concatenate(
        [
            offsets,
            rates,
            high(rate_sum).astype(jnp.float32),
            low(rate_sum).astype(jnp.float32),
            high(speed).astype(jnp.float32),
            low(speed).astype(jnp.float32),
        ],
        axis=0,
    )
    wide_pair_ref[rows:] = coef_ref[:, pl.ds(wide_first, HALO)].astype(jnp.bfloat16)
    near_pair_ref[rows:] = coef_ref[:, pl.ds(near_first, HALO)].astype(jnp.bfloat16)
    for i, copy in enumerate(large):
        copy.wait()
        part = pl.ds(i * chunk, chunk)
        wide_pair_ref[part] = state_ref[part, pl.ds(wide_first, HALO)].astype(jnp.bfloat16)
        near_pair_ref[part] = state_ref[part, pl.ds(near_first, HALO)].astype(jnp.bfloat16)


def vmem(count):
    return [pl.BlockSpec(memory_space=pltpu.VMEM)] * count


def in_vmem(*values):
    return [pltpu.with_memory_space_constraint(value, pltpu.VMEM) for value in values]


def in_hbm(*values):
    return [pltpu.with_memory_space_constraint(value, pltpu.HBM) for value in values]


def prepare(state, columns, rates, speed, total):
    rows, cells = state.shape
    side = pltpu.VMEM((rows + COEF_ROWS, HALO), jnp.bfloat16)
    return pl.pallas_call(
        functools.partial(prepare_kernel, total=total),
        out_shape=(
            side,
            side,
            pltpu.VMEM((rows, cells), jnp.float32),
            pltpu.VMEM((COEF_ROWS, cells), jnp.float32),
        ),
        in_specs=[pl.BlockSpec(memory_space=pltpu.HBM)] * 4,
        out_specs=tuple(vmem(4)),
        scratch_shapes=[
            pltpu.VMEM(columns.shape, jnp.int32),
            pltpu.VMEM(rates.shape, jnp.float32),
            pltpu.VMEM(speed.shape, jnp.float32),
            pltpu.SemaphoreType.DMA((3,)),
            pltpu.SemaphoreType.DMA((STATE_CHUNKS,)),
        ],
        compiler_params=pltpu.CompilerParams(vmem_limit_bytes=8 << 20),
        name="prepare",
    )(*in_hbm(state, columns, rates, speed))


def matrices_kernel(coef_ref, matrix_ref):
    for b in range(matrix_ref.shape[0]):
        part = slice(b * BLOCK, (b + 1) * BLOCK)
        build_matrix(matrix_ref, b, coef_ref[0:6, part], coef_ref[6:12, part])


def own_matrices(coef):
    shape = (coef.shape[1] // BLOCK, WINDOW, BLOCK)
    return pl.pallas_call(
        matrices_kernel,
        out_shape=pltpu.VMEM(shape, jnp.bfloat16),
        in_specs=vmem(1),
        out_specs=vmem(1)[0],
        compiler_params=pltpu.CompilerParams(vmem_limit_bytes=4 << 20),
        name="own_matrices",
    )(*in_vmem(coef))


def message_kernel(
    patch_hbm, row_hbm, value_hbm, error_hbm, message_ref,
    patch_ref, row_ref, value_ref, error_ref, sem, *, regions, groups,
):
    small = fetches(
        (patch_hbm, row_hbm, value_hbm, error_hbm), (patch_ref, row_ref, value_ref, error_ref), sem
    )
    for copy in small:
        copy.start()
    for copy in small:
        copy.wait()
    devices, count = message_ref.shape[0], patch_ref.shape[1]
    target = lax.broadcasted_iota(jnp.int32, (devices, count), 0)
    wanted = target % regions * groups + target // regions
    hit = jnp.where(patch_ref[...] == wanted, 1.0, 0.0)
    before = lax.broadcasted_iota(jnp.int32, (count, count), 0)
    after = lax.broadcasted_iota(jnp.int32, (count, count), 1)
    earlier = jnp.where(before < after, 1.0, 0.0).astype(jnp.bfloat16)
    rank = dot_f32(hit.astype(jnp.bfloat16), earlier)
    field = lax.broadcasted_iota(jnp.int32, (message_ref.shape[1], count), 0)
    location = row_ref[...].astype(jnp.float32) + 1.0
    weight = 1.0 / (error_ref[...] * error_ref[...])
    message = None
    for slot in range(2):
        chosen = jnp.where(rank == float(slot), hit, 0.0).astype(jnp.bfloat16)
        values = jnp.zeros(field.shape, jnp.float32)
        for k, item in enumerate((location, value_ref[...], weight)):
            values = jnp.where(field == 3 * slot + k, item, values)
        for _ in range(3):
            piece = high(values)
            values = values - piece.astype(jnp.float32)
            term = dot_f32(chosen, piece, (((1,), (1,)), ((), ())))
            message = term if message is None else message + term
    message_ref[...] = message


def observation_message(patch, row, value, error, regions, groups):
    count = patch.shape[1]
    return pl.pallas_call(
        functools.partial(message_kernel, regions=regions, groups=groups),
        out_shape=jax.ShapeDtypeStruct((regions * groups, TILE), jnp.float32),
        in_specs=[pl.BlockSpec(memory_space=pltpu.HBM)] * 4,
        out_specs=vmem(1)[0],
        scratch_shapes=[
            pltpu.VMEM((1, count), jnp.int32),
            pltpu.VMEM((1, count), jnp.int32),
            pltpu.VMEM((1, count), jnp.float32),
            pltpu.VMEM((1, count), jnp.float32),
            pltpu.SemaphoreType.DMA((4,)),
        ],
        compiler_params=pltpu.CompilerParams(vmem_limit_bytes=4 << 20),
        name="message",
    )(*in_hbm(patch, row, value, error))


def forecast_kernel(
    state_ref, wide_pair_ref, near_pair_ref, own_ref, own_coef_ref, own_0, own_1, own_2, own_3,
    swap_ref, matrix_ref, coef_ref, field_a, field_b, wide_ref,
):
    rows, cells = state_ref.shape
    own_blocks = cells // BLOCK
    side_blocks = (STEPS - 1) * RIM // BLOCK
    blocks = own_blocks + 2 * side_blocks
    odd = lax.axis_index("region") % 2
    far = HALO + cells
    for ref, begin in ((wide_pair_ref, odd * far), (near_pair_ref, (1 - odd) * far)):
        begin = pl.multiple_of(begin, TILE)
        coef_ref[:, pl.ds(begin, HALO)] = ref[rows:].astype(jnp.float32)
        field_a[:, pl.ds(begin, HALO)] = ref[:rows]
    coef_ref[:, HALO:far] = own_coef_ref[...]
    field_a[:, HALO:far] = state_ref[...].astype(jnp.bfloat16)
    keep, speed, matrices = [], [], []
    for b in range(blocks):
        part = slice(RIM + b * BLOCK, RIM + (b + 1) * BLOCK)
        if side_blocks <= b < side_blocks + own_blocks:
            matrices.append((own_ref, b - side_blocks))
        else:
            index = b if b < side_blocks else b - own_blocks
            build_matrix(matrix_ref, index, coef_ref[0:6, part], coef_ref[6:12, part])
            matrices.append((matrix_ref, index))
        keep.append(1.0 - (coef_ref[12:13, part] + coef_ref[13:14, part]))
        speed.append(coef_ref[14:15, part] + coef_ref[15:16, part])
    source, target = field_a, field_b
    for step in range(STEPS - 1):
        for b in range(step, blocks - step):
            first = b * BLOCK
            middle = slice(first + RIM, first + RIM + BLOCK)
            holder, index = matrices[b]
            summed = dot_f32(source[:, first : first + WINDOW], holder[index])
            if step > 0:
                centre = wide_ref[:, middle]
            elif side_blocks <= b < side_blocks + own_blocks:
                own = (b - side_blocks) * BLOCK
                centre = state_ref[:, own : own + BLOCK]
            else:
                centre = source[:, middle].astype(jnp.float32)
            blended = centre * keep[b] + summed
            result = blended + speed[b] * jnp.tanh(blended)
            wide_ref[:, middle] = result
            target[:, middle] = result.astype(jnp.bfloat16)
        source, target = target, source
    member = lax.axis_index("member")
    row, core = member // 2, member % 2
    for shift, own_out in enumerate((own_0, own_1, own_2, own_3)):
        block = (row + shift) % own_blocks
        first = pl.multiple_of(block * BLOCK + (HALO - RIM), TILE)
        middle = pl.ds(pl.multiple_of(block * BLOCK + HALO, TILE), BLOCK)
        summed = dot_f32(source[:, pl.ds(first, WINDOW)], own_ref[block])
        kept = 1.0 - (coef_ref[12:13, middle] + coef_ref[13:14, middle])
        quick = coef_ref[14:15, middle] + coef_ref[15:16, middle]
        blended = wide_ref[:, middle] * kept + summed
        result = (blended + quick * jnp.tanh(blended)).astype(jnp.bfloat16)
        even, odd_half = result[:, :PATCH_CELLS], result[:, PATCH_CELLS:]
        own_out[...] = jnp.where(core == 0, even, odd_half)
        swap_ref[shift] = jnp.where(core == 0, odd_half, even)


def exchange_shapes(rows):
    return (pltpu.VMEM((rows, PATCH_CELLS), jnp.bfloat16),) * SHIFTS + (
        pltpu.VMEM((SHIFTS, rows, PATCH_CELLS), jnp.bfloat16),
    )


def forecast(state, wide_pair, near_pair, own, coef):
    rows, cells = state.shape
    sides = 2 * (STEPS - 1) * RIM // BLOCK
    padded = cells + 2 * HALO
    return pl.pallas_call(
        forecast_kernel,
        out_shape=exchange_shapes(rows),
        in_specs=vmem(5),
        out_specs=tuple(vmem(SHIFTS + 1)),
        scratch_shapes=[
            pltpu.VMEM((sides, WINDOW, BLOCK), jnp.bfloat16),
            pltpu.VMEM((COEF_ROWS, padded), jnp.float32),
            pltpu.VMEM((rows, padded), jnp.bfloat16),
            pltpu.VMEM((rows, padded), jnp.bfloat16),
            pltpu.VMEM((rows, padded), jnp.float32),
        ],
        compiler_params=pltpu.CompilerParams(vmem_limit_bytes=16 << 20),
        name="forecast",
    )(*in_vmem(state, wide_pair, near_pair, own, coef))


def merge_kernel(own_1, own_2, own_3, got_ref, out_1, out_2, out_3):
    for shift, own, out in ((1, own_1, out_1), (2, own_2, out_2), (3, own_3, out_3)):
        out[0] = own[...]
        out[1] = got_ref[shift]


def exchange(parts, sign):
    rows = parts[0].shape[0]
    groups = lax.axis_size("member")
    got = lax.ppermute(parts[SHIFTS], "member", [(i, i ^ 1) for i in range(groups)])
    merged = pl.pallas_call(
        merge_kernel,
        out_shape=(pltpu.VMEM((2, rows, PATCH_CELLS), jnp.bfloat16),) * (SHIFTS - 1),
        in_specs=vmem(SHIFTS),
        out_specs=tuple(vmem(SHIFTS - 1)),
        compiler_params=pltpu.CompilerParams(vmem_limit_bytes=2 << 20),
        name="merge",
    )(*in_vmem(*parts[1:SHIFTS], got))
    moved = [None] * (SHIFTS - 1)
    for shift in (2, 1, 3):
        edges = [(i, (i + sign * 2 * shift) % groups) for i in range(groups)]
        moved[shift - 1] = lax.ppermute(merged[shift - 1], "member", edges)
    return parts[0], got, *moved


def analysis_kernel(
    self_ref, got_ref, from_1, from_2, from_3, message_ref, own_0, own_1, own_2, own_3, swap_ref,
    wide_ref, x2_ref, select_ref,
):
    rows = self_ref.shape[0]
    members = wide_ref.shape[0] // LEVELS
    span = LEVELS * PATCH_CELLS
    arrived = [self_ref[...], got_ref[0]]
    for ref in (from_1, from_2, from_3):
        arrived += [ref[0], ref[1]]
    for i, piece in enumerate(arrived):
        wide_ref[i * rows : (i + 1) * rows] = piece.astype(jnp.float32)
    for level in range(LEVELS):
        part = wide_ref[pl.ds(level, members, stride=LEVELS), :]
        x2_ref[:, level * PATCH_CELLS : (level + 1) * PATCH_CELLS] = part.astype(jnp.bfloat16)
    message = jnp.transpose(message_ref[...])
    location = jnp.concatenate([message[0:1], message[3:4]], axis=1) - 1.0
    value = jnp.concatenate([message[1:2], message[4:5]], axis=1)
    weight = jnp.concatenate([message[2:3], message[5:6]], axis=1)
    slots = location.shape[1]
    location = location.astype(jnp.int32)
    for first in range(0, span, PATCH_CELLS):
        row = lax.broadcasted_iota(jnp.int32, (PATCH_CELLS, slots), 0) + first
        hot = jnp.where(row == location, 1.0, 0.0)
        select_ref[first : first + PATCH_CELLS, :] = hot.astype(jnp.bfloat16)
    seen = dot_f32(x2_ref[...], select_ref[...])
    seen_mean = jnp.sum(seen, axis=0, keepdims=True) * (1.0 / members)
    rooted = jnp.sqrt(weight)
    spread = 1.0 / math.sqrt(members - 1.0)
    scaled = (seen - seen_mean) * (rooted * spread)
    row = lax.broadcasted_iota(jnp.int32, (members, members), 0)
    column = lax.broadcasted_iota(jnp.int32, (members, members), 1)
    diagonal = jnp.where(row == column, 1.0, 0.0)
    product = dot_half(scaled, scaled, (((1,), (1,)), ((), ())))
    system = diagonal + product
    square = jnp.sum(jnp.sum(system * system, axis=0, keepdims=True), axis=1, keepdims=True)
    inverse_scale = jnp.broadcast_to(lax.rsqrt(square), (1, members))
    innovation = rooted * (value - seen_mean) * spread
    forcing = jnp.sum(scaled * innovation, axis=1, keepdims=True)
    p, z = inverse_scale, jnp.ones_like(inverse_scale)
    both = product * inverse_scale
    root = None
    for sweep in range(NS_ITERS):
        f = 1.5 - 0.5 * p
        factor = -0.5 * both
        narrow = factor.astype(jnp.bfloat16)
        if root is None:
            new_root = factor
        else:
            new_root = z * factor + f * root + dot_f32(high(root), narrow)
        if sweep < NS_ITERS - 1:
            once = p * factor + f * both + dot_f32(high(both), narrow)
            q = p * f
            both = q * factor + f * once + dot_f32(high(once), narrow)
            p = q * f
        root, z = new_root, z * f
    whole = root + z * diagonal
    inner = jnp.sum(whole * forcing, axis=0, keepdims=True)
    shift = jnp.sum(whole * inner, axis=1, keepdims=True) * inverse_scale[:, 0:1]
    half_scale = jnp.sqrt(inverse_scale)
    transform = (root * half_scale).astype(jnp.bfloat16)
    direct = (z * half_scale)[:, 0:PATCH_CELLS]
    pair = 2
    for level in range(0, LEVELS, pair):
        pieces = []
        for k in range(level, level + pair):
            part = x2_ref[:, k * PATCH_CELLS : (k + 1) * PATCH_CELLS].astype(jnp.float32)
            mean = jnp.sum(part, axis=0, keepdims=True) * (1.0 / members)
            anomaly = part - mean
            base = mean + jnp.sum(anomaly * shift, axis=0, keepdims=True) + direct * anomaly
            pieces.append((anomaly.astype(jnp.bfloat16), base))
        moved = dot_f32(transform, jnp.concatenate([piece[0] for piece in pieces], axis=1))
        for k in range(pair):
            updated = pieces[k][1] + moved[:, k * PATCH_CELLS : (k + 1) * PATCH_CELLS]
            wide_ref[pl.ds(level + k, members, stride=LEVELS), :] = updated
    for shift, own in enumerate((own_0, own_1, own_2, own_3)):
        first = 2 * shift * rows
        own[...] = wide_ref[first : first + rows].astype(jnp.bfloat16)
        swap_ref[shift] = wide_ref[first + rows : first + 2 * rows].astype(jnp.bfloat16)


def analysis(received, message):
    rows = received[0].shape[0]
    wide = 2 * SHIFTS * rows
    members = wide // LEVELS
    slots = 2 * message.shape[0]
    return pl.pallas_call(
        analysis_kernel,
        out_shape=exchange_shapes(rows),
        in_specs=vmem(SHIFTS + 2),
        out_specs=tuple(vmem(SHIFTS + 1)),
        compiler_params=pltpu.CompilerParams(vmem_limit_bytes=12 << 20),
        scratch_shapes=[
            pltpu.VMEM((wide, PATCH_CELLS), jnp.float32),
            pltpu.VMEM((members, LEVELS * PATCH_CELLS), jnp.bfloat16),
            pltpu.VMEM((LEVELS * PATCH_CELLS, slots), jnp.bfloat16),
        ],
        name="analysis",
    )(*in_vmem(*received, message))


def place_kernel(self_ref, got_ref, from_1, from_2, from_3, out_hbm, sem):
    member = lax.axis_index("member")
    row, core = member // 2, member % 2
    copies = []
    pieces = [self_ref, got_ref.at[0]]
    for ref in (from_1, from_2, from_3):
        pieces += [ref.at[0], ref.at[1]]
    for i, piece in enumerate(pieces):
        patch = (row + i // 2) % SHIFTS * 2 + (core + i) % 2
        lanes = pl.ds(pl.multiple_of(patch * PATCH_CELLS, PATCH_CELLS), PATCH_CELLS)
        copies.append(pltpu.make_async_copy(piece, out_hbm.at[:, lanes], sem.at[i]))
    for copy in copies:
        copy.start()
    for copy in copies:
        copy.wait()


def place(received, cells):
    rows = received[0].shape[0]
    return pl.pallas_call(
        place_kernel,
        out_shape=jax.ShapeDtypeStruct((rows, cells), jnp.bfloat16),
        in_specs=vmem(SHIFTS + 1),
        out_specs=pl.BlockSpec(memory_space=pltpu.HBM),
        scratch_shapes=[pltpu.SemaphoreType.DMA((2 * SHIFTS,))],
        compiler_params=pltpu.CompilerParams(vmem_limit_bytes=2 << 20),
        name="place",
    )(*in_vmem(*received))


def on_device(
    state, adjacent_columns, adjacent_rates, amplification_speed,
    obs_patch, obs_row, obs_value, obs_error,
):
    members, levels, cells = state.shape
    regions = lax.axis_size("region")
    groups = lax.axis_size("member")
    total = cells * regions
    flat = state.reshape(members * levels, cells)
    wide_pair, near_pair, kept, coef = prepare(
        flat, adjacent_columns, adjacent_rates, amplification_speed[None, :], total
    )
    pairs = [(i, (i + 1) % regions) for i in range(regions)]
    wide_swap = [edge for i, j in pairs[1::2] for edge in ((i, j), (j, i))]
    near_swap = [edge for i, j in pairs[0::2] for edge in ((i, j), (j, i))]
    near_pair = lax.ppermute(near_pair, "region", near_swap)
    wide_pair = lax.ppermute(wide_pair, "region", wide_swap)
    message = observation_message(
        obs_patch[None, :], obs_row[None, :], obs_value[None, :], obs_error[None, :],
        regions, groups,
    )
    message = lax.all_to_all(message, ("member", "region"), 0, 0, tiled=True)
    own = own_matrices(coef)
    parts = forecast(kept, wide_pair, near_pair, own, coef)
    received = exchange(parts, 1)
    back = exchange(analysis(received, message), -1)
    return place(back, cells).reshape(members, levels, cells)


def solution(mesh):
    placed = (
        P("member", None, "region"),
        P(None, "region"),
        P(None, "region"),
        P("region"),
        P(("member", "region")),
        P(("member", "region")),
        P(("member", "region")),
        P(("member", "region")),
    )

    return jax.shard_map(
        on_device, mesh=mesh, in_specs=placed, out_specs=P("member", None, "region"), check_vma=False
    )
```

```python
import functools
import math

import jax
import jax.numpy as jnp
from jax import lax
from jax.experimental import pallas as pl
from jax.experimental.pallas import tpu as pltpu
from jax.sharding import PartitionSpec as P


PATCH_CELLS = 128
RIM = 256
STEPS = 3
NS_ITERS = 6
LEVELS = 8
BLOCK = 256
WINDOW = BLOCK + 2 * RIM
HALO = STEPS * RIM
COEF_ROWS = 16
TILE = 128
STATE_CHUNKS = 4
SHIFTS = 4


def high(value):
    return value.astype(jnp.bfloat16)


def low(value):
    return (value - high(value).astype(jnp.float32)).astype(jnp.bfloat16)


def dot_f32(a, b, dims=(((1,), (0,)), ((), ()))):
    return lax.dot_general(a, b, dims, preferred_element_type=jnp.float32)


def dot_half(a, b, dims=(((1,), (0,)), ((), ()))):
    return dot_f32(high(a), high(b), dims)


def cell_offsets(columns, first, total):
    cell = first + lax.broadcasted_iota(jnp.int32, columns.shape, 1)
    offset = columns - cell
    offset = jnp.where(offset > total // 2, offset - total, offset)
    return jnp.where(offset < -(total // 2), offset + total, offset)


def build_matrix(matrix_ref, index, offsets, rates):
    zero = jnp.zeros((TILE, TILE), jnp.bfloat16)
    row = lax.broadcasted_iota(jnp.int32, (TILE, TILE), 0).astype(jnp.float32)
    row = row.astype(jnp.bfloat16)
    lane = lax.broadcasted_iota(jnp.int32, (1, TILE), 1).astype(jnp.float32)
    reach = (TILE + 2 * RIM) // TILE
    for part in range(BLOCK // TILE):
        lanes = slice(part * TILE, (part + 1) * TILE)
        local = offsets[:, lanes] + (lane + float(RIM))
        rate = [
            jnp.broadcast_to(rates[k : k + 1, lanes].astype(jnp.bfloat16), (TILE, TILE))
            for k in range(6)
        ]
        for tile in range(WINDOW // TILE):
            rows = slice(tile * TILE, (tile + 1) * TILE)
            step = tile - part
            if step < 0 or step >= reach:
                matrix_ref[index, rows, lanes] = zero
                continue
            total = None
            for k in range(6):
                near = (local[k : k + 1] - float(step * TILE)).astype(jnp.bfloat16)
                hit = row == jnp.broadcast_to(near, (TILE, TILE))
                term = jnp.where(hit, rate[k], zero)
                total = term if total is None else total + term
            matrix_ref[index, rows, lanes] = total


def fetches(sources, targets, sem):
    return [
        pltpu.make_async_copy(source, target, sem.at[i])
        for i, (source, target) in enumerate(zip(sources, targets))
    ]


def prepare_kernel(
    state_hbm, column_hbm, rate_hbm, speed_hbm, patch_hbm, row_hbm, value_hbm, error_hbm,
    up_ref, down_ref, state_ref, coef_ref, patch_ref, row_ref, value_ref, error_ref,
    column_ref, rate_ref, speed_ref, small_sem, later_sem, state_sem, *, total,
):
    rows, cells = state_ref.shape
    small = fetches(
        (column_hbm, rate_hbm, speed_hbm), (column_ref, rate_ref, speed_ref), small_sem
    )
    later = fetches(
        (patch_hbm, row_hbm, value_hbm, error_hbm),
        (patch_ref, row_ref, value_ref, error_ref),
        later_sem,
    )
    chunk = rows // STATE_CHUNKS
    large = [
        pltpu.make_async_copy(
            state_hbm.at[pl.ds(i * chunk, chunk)],
            state_ref.at[pl.ds(i * chunk, chunk)],
            state_sem.at[i],
        )
        for i in range(STATE_CHUNKS)
    ]
    for copy in small + large + later:
        copy.start()
    for copy in small:
        copy.wait()
    region = lax.axis_index("region")
    last = cells - HALO
    offsets = cell_offsets(column_ref[...], region * cells, total).astype(jnp.float32)
    rates = rate_ref[...]
    rate_sum = jnp.sum(rates, axis=0, keepdims=True)
    speed = speed_ref[...]
    coef_ref[...] = jnp.concatenate(
        [
            offsets,
            rates,
            high(rate_sum).astype(jnp.float32),
            low(rate_sum).astype(jnp.float32),
            high(speed).astype(jnp.float32),
            low(speed).astype(jnp.float32),
        ],
        axis=0,
    )
    up_ref[rows:] = coef_ref[:, last:].astype(jnp.bfloat16)
    down_ref[rows:] = coef_ref[:, :HALO].astype(jnp.bfloat16)
    for i, copy in enumerate(large):
        copy.wait()
        part = pl.ds(i * chunk, chunk)
        up_ref[part] = state_ref[part, last:].astype(jnp.bfloat16)
        down_ref[part] = state_ref[part, :HALO].astype(jnp.bfloat16)
    for copy in later:
        copy.wait()


def vmem(count):
    return [pl.BlockSpec(memory_space=pltpu.VMEM)] * count


def in_vmem(*values):
    return [pltpu.with_memory_space_constraint(value, pltpu.VMEM) for value in values]


def in_hbm(*values):
    return [pltpu.with_memory_space_constraint(value, pltpu.HBM) for value in values]


def prepare(state, columns, rates, speed, patch, row, value, error, total):
    rows, cells = state.shape
    side = pltpu.VMEM((rows + COEF_ROWS, HALO), jnp.bfloat16)
    return pl.pallas_call(
        functools.partial(prepare_kernel, total=total),
        out_shape=(
            side,
            side,
            pltpu.VMEM((rows, cells), jnp.float32),
            pltpu.VMEM((COEF_ROWS, cells), jnp.float32),
            *(pltpu.VMEM(item.shape, item.dtype) for item in (patch, row, value, error)),
        ),
        in_specs=[pl.BlockSpec(memory_space=pltpu.HBM)] * 8,
        out_specs=tuple(vmem(8)),
        scratch_shapes=[
            pltpu.VMEM(columns.shape, jnp.int32),
            pltpu.VMEM(rates.shape, jnp.float32),
            pltpu.VMEM(speed.shape, jnp.float32),
            pltpu.SemaphoreType.DMA((3,)),
            pltpu.SemaphoreType.DMA((4,)),
            pltpu.SemaphoreType.DMA((STATE_CHUNKS,)),
        ],
        compiler_params=pltpu.CompilerParams(vmem_limit_bytes=8 << 20),
        name="prepare",
    )(*in_hbm(state, columns, rates, speed, patch, row, value, error))


def matrices_kernel(coef_ref, matrix_ref):
    for b in range(matrix_ref.shape[0]):
        part = slice(b * BLOCK, (b + 1) * BLOCK)
        build_matrix(matrix_ref, b, coef_ref[0:6, part], coef_ref[6:12, part])


def own_matrices(coef):
    shape = (coef.shape[1] // BLOCK, WINDOW, BLOCK)
    return pl.pallas_call(
        matrices_kernel,
        out_shape=pltpu.VMEM(shape, jnp.bfloat16),
        in_specs=vmem(1),
        out_specs=vmem(1)[0],
        compiler_params=pltpu.CompilerParams(vmem_limit_bytes=4 << 20),
        name="own_matrices",
    )(*in_vmem(coef))


def message_kernel(patch_ref, row_ref, value_ref, error_ref, message_ref, *, regions, groups):
    devices, count = message_ref.shape[0], patch_ref.shape[1]
    target = lax.broadcasted_iota(jnp.int32, (devices, count), 0)
    wanted = target % regions * groups + target // regions
    hit = jnp.where(patch_ref[...] == wanted, 1.0, 0.0)
    before = lax.broadcasted_iota(jnp.int32, (count, count), 0)
    after = lax.broadcasted_iota(jnp.int32, (count, count), 1)
    earlier = jnp.where(before < after, 1.0, 0.0).astype(jnp.bfloat16)
    rank = dot_f32(hit.astype(jnp.bfloat16), earlier)
    field = lax.broadcasted_iota(jnp.int32, (message_ref.shape[1], count), 0)
    location = row_ref[...].astype(jnp.float32) + 1.0
    weight = 1.0 / (error_ref[...] * error_ref[...])
    message = None
    for slot in range(2):
        chosen = jnp.where(rank == float(slot), hit, 0.0).astype(jnp.bfloat16)
        values = jnp.zeros(field.shape, jnp.float32)
        for k, item in enumerate((location, value_ref[...], weight)):
            values = jnp.where(field == 3 * slot + k, item, values)
        for _ in range(3):
            piece = high(values)
            values = values - piece.astype(jnp.float32)
            term = dot_f32(chosen, piece, (((1,), (1,)), ((), ())))
            message = term if message is None else message + term
    message_ref[...] = message


def observation_message(patch, row, value, error, regions, groups):
    return pl.pallas_call(
        functools.partial(message_kernel, regions=regions, groups=groups),
        out_shape=jax.ShapeDtypeStruct((regions * groups, TILE), jnp.float32),
        in_specs=vmem(4),
        out_specs=vmem(1)[0],
        compiler_params=pltpu.CompilerParams(vmem_limit_bytes=4 << 20),
        name="message",
    )(*in_vmem(patch, row, value, error))


def forecast_kernel(
    state_ref, left_ref, right_ref, own_ref, own_coef_ref, own_0, own_1, own_2, own_3,
    swap_ref, matrix_ref, coef_ref, field_a, field_b, wide_ref,
):
    rows, cells = state_ref.shape
    own_blocks = cells // BLOCK
    side_blocks = (STEPS - 1) * RIM // BLOCK
    blocks = own_blocks + 2 * side_blocks
    far = HALO + cells
    for ref, begin in ((left_ref, 0), (right_ref, far)):
        coef_ref[:, begin : begin + HALO] = ref[rows:].astype(jnp.float32)
        field_a[:, begin : begin + HALO] = ref[:rows]
    coef_ref[:, HALO:far] = own_coef_ref[...]
    field_a[:, HALO:far] = state_ref[...].astype(jnp.bfloat16)
    keep, speed, matrices = [], [], []
    for b in range(blocks):
        part = slice(RIM + b * BLOCK, RIM + (b + 1) * BLOCK)
        if side_blocks <= b < side_blocks + own_blocks:
            matrices.append((own_ref, b - side_blocks))
        else:
            index = b if b < side_blocks else b - own_blocks
            build_matrix(matrix_ref, index, coef_ref[0:6, part], coef_ref[6:12, part])
            matrices.append((matrix_ref, index))
        keep.append(1.0 - (coef_ref[12:13, part] + coef_ref[13:14, part]))
        speed.append(coef_ref[14:15, part] + coef_ref[15:16, part])
    source, target = field_a, field_b
    for step in range(STEPS - 1):
        for b in range(step, blocks - step):
            first = b * BLOCK
            middle = slice(first + RIM, first + RIM + BLOCK)
            holder, index = matrices[b]
            summed = dot_f32(source[:, first : first + WINDOW], holder[index])
            if step > 0:
                centre = wide_ref[:, middle]
            elif side_blocks <= b < side_blocks + own_blocks:
                own = (b - side_blocks) * BLOCK
                centre = state_ref[:, own : own + BLOCK]
            else:
                centre = source[:, middle].astype(jnp.float32)
            blended = centre * keep[b] + summed
            result = blended + speed[b] * jnp.tanh(blended)
            wide_ref[:, middle] = result
            target[:, middle] = result.astype(jnp.bfloat16)
        source, target = target, source
    member = lax.axis_index("member")
    row, core = member // 2, member % 2
    for shift, own_out in enumerate((own_0, own_1, own_2, own_3)):
        block = (row + shift) % own_blocks
        first = pl.multiple_of(block * BLOCK + (HALO - RIM), TILE)
        middle = pl.ds(pl.multiple_of(block * BLOCK + HALO, TILE), BLOCK)
        summed = dot_f32(source[:, pl.ds(first, WINDOW)], own_ref[block])
        kept = 1.0 - (coef_ref[12:13, middle] + coef_ref[13:14, middle])
        quick = coef_ref[14:15, middle] + coef_ref[15:16, middle]
        blended = wide_ref[:, middle] * kept + summed
        result = (blended + quick * jnp.tanh(blended)).astype(jnp.bfloat16)
        even, odd_half = result[:, :PATCH_CELLS], result[:, PATCH_CELLS:]
        own_out[...] = jnp.where(core == 0, even, odd_half)
        swap_ref[shift] = jnp.where(core == 0, odd_half, even)


def exchange_shapes(rows):
    return (pltpu.VMEM((rows, PATCH_CELLS), jnp.bfloat16),) * SHIFTS + (
        pltpu.VMEM((SHIFTS, rows, PATCH_CELLS), jnp.bfloat16),
    )


def forecast(state, left, right, own, coef):
    rows, cells = state.shape
    sides = 2 * (STEPS - 1) * RIM // BLOCK
    padded = cells + 2 * HALO
    return pl.pallas_call(
        forecast_kernel,
        out_shape=exchange_shapes(rows),
        in_specs=vmem(5),
        out_specs=tuple(vmem(SHIFTS + 1)),
        scratch_shapes=[
            pltpu.VMEM((sides, WINDOW, BLOCK), jnp.bfloat16),
            pltpu.VMEM((COEF_ROWS, padded), jnp.float32),
            pltpu.VMEM((rows, padded), jnp.bfloat16),
            pltpu.VMEM((rows, padded), jnp.bfloat16),
            pltpu.VMEM((rows, padded), jnp.float32),
        ],
        compiler_params=pltpu.CompilerParams(vmem_limit_bytes=16 << 20),
        name="forecast",
    )(*in_vmem(state, left, right, own, coef))


def merge_kernel(own_1, own_2, own_3, got_ref, out_1, out_2, out_3):
    for shift, own, out in ((1, own_1, out_1), (2, own_2, out_2), (3, own_3, out_3)):
        out[0] = own[...]
        out[1] = got_ref[shift]


def exchange(parts, sign):
    rows = parts[0].shape[0]
    groups = lax.axis_size("member")
    got = lax.ppermute(parts[SHIFTS], "member", [(i, i ^ 1) for i in range(groups)])
    merged = pl.pallas_call(
        merge_kernel,
        out_shape=(pltpu.VMEM((2, rows, PATCH_CELLS), jnp.bfloat16),) * (SHIFTS - 1),
        in_specs=vmem(SHIFTS),
        out_specs=tuple(vmem(SHIFTS - 1)),
        compiler_params=pltpu.CompilerParams(vmem_limit_bytes=2 << 20),
        name="merge",
    )(*in_vmem(*parts[1:SHIFTS], got))
    moved = [None] * (SHIFTS - 1)
    for shift in (2, 1, 3):
        edges = [(i, (i + sign * 2 * shift) % groups) for i in range(groups)]
        moved[shift - 1] = lax.ppermute(merged[shift - 1], "member", edges)
    return parts[0], got, *moved


def analysis_kernel(
    self_ref, got_ref, from_1, from_2, from_3, message_ref, own_0, own_1, own_2, own_3, swap_ref,
    wide_ref, x2_ref, select_ref,
):
    rows = self_ref.shape[0]
    members = wide_ref.shape[0] // LEVELS
    span = LEVELS * PATCH_CELLS
    arrived = [self_ref[...], got_ref[0]]
    for ref in (from_1, from_2, from_3):
        arrived += [ref[0], ref[1]]
    for i, piece in enumerate(arrived):
        wide_ref[i * rows : (i + 1) * rows] = piece.astype(jnp.float32)
    for level in range(LEVELS):
        part = wide_ref[pl.ds(level, members, stride=LEVELS), :]
        x2_ref[:, level * PATCH_CELLS : (level + 1) * PATCH_CELLS] = part.astype(jnp.bfloat16)
    message = jnp.transpose(message_ref[...])
    location = jnp.concatenate([message[0:1], message[3:4]], axis=1) - 1.0
    value = jnp.concatenate([message[1:2], message[4:5]], axis=1)
    weight = jnp.concatenate([message[2:3], message[5:6]], axis=1)
    slots = location.shape[1]
    location = location.astype(jnp.int32)
    for first in range(0, span, PATCH_CELLS):
        row = lax.broadcasted_iota(jnp.int32, (PATCH_CELLS, slots), 0) + first
        hot = jnp.where(row == location, 1.0, 0.0)
        select_ref[first : first + PATCH_CELLS, :] = hot.astype(jnp.bfloat16)
    seen = dot_f32(x2_ref[...], select_ref[...])
    seen_mean = jnp.sum(seen, axis=0, keepdims=True) * (1.0 / members)
    rooted = jnp.sqrt(weight)
    spread = 1.0 / math.sqrt(members - 1.0)
    scaled = (seen - seen_mean) * (rooted * spread)
    row = lax.broadcasted_iota(jnp.int32, (members, members), 0)
    column = lax.broadcasted_iota(jnp.int32, (members, members), 1)
    diagonal = jnp.where(row == column, 1.0, 0.0)
    product = dot_half(scaled, scaled, (((1,), (1,)), ((), ())))
    system = diagonal + product
    square = jnp.sum(jnp.sum(system * system, axis=0, keepdims=True), axis=1, keepdims=True)
    inverse_scale = jnp.broadcast_to(lax.rsqrt(square), (1, members))
    innovation = rooted * (value - seen_mean) * spread
    forcing = jnp.sum(scaled * innovation, axis=1, keepdims=True)
    p, z = inverse_scale, jnp.ones_like(inverse_scale)
    both = product * inverse_scale
    root = None
    for sweep in range(NS_ITERS):
        f = 1.5 - 0.5 * p
        factor = -0.5 * both
        narrow = factor.astype(jnp.bfloat16)
        if root is None:
            new_root = factor
        else:
            new_root = z * factor + f * root + dot_f32(high(root), narrow)
        if sweep < NS_ITERS - 1:
            once = p * factor + f * both + dot_f32(high(both), narrow)
            q = p * f
            both = q * factor + f * once + dot_f32(high(once), narrow)
            p = q * f
        root, z = new_root, z * f
    whole = root + z * diagonal
    inner = jnp.sum(whole * forcing, axis=0, keepdims=True)
    shift = jnp.sum(whole * inner, axis=1, keepdims=True) * inverse_scale[:, 0:1]
    half_scale = jnp.sqrt(inverse_scale)
    transform = (root * half_scale).astype(jnp.bfloat16)
    direct = (z * half_scale)[:, 0:PATCH_CELLS]
    pair = 2
    for level in range(0, LEVELS, pair):
        pieces = []
        for k in range(level, level + pair):
            part = x2_ref[:, k * PATCH_CELLS : (k + 1) * PATCH_CELLS].astype(jnp.float32)
            mean = jnp.sum(part, axis=0, keepdims=True) * (1.0 / members)
            anomaly = part - mean
            base = mean + jnp.sum(anomaly * shift, axis=0, keepdims=True) + direct * anomaly
            pieces.append((anomaly.astype(jnp.bfloat16), base))
        moved = dot_f32(transform, jnp.concatenate([piece[0] for piece in pieces], axis=1))
        for k in range(pair):
            updated = pieces[k][1] + moved[:, k * PATCH_CELLS : (k + 1) * PATCH_CELLS]
            wide_ref[pl.ds(level + k, members, stride=LEVELS), :] = updated
    for shift, own in enumerate((own_0, own_1, own_2, own_3)):
        first = 2 * shift * rows
        own[...] = wide_ref[first : first + rows].astype(jnp.bfloat16)
        swap_ref[shift] = wide_ref[first + rows : first + 2 * rows].astype(jnp.bfloat16)


def analysis(received, message):
    rows = received[0].shape[0]
    wide = 2 * SHIFTS * rows
    members = wide // LEVELS
    slots = 2 * message.shape[0]
    return pl.pallas_call(
        analysis_kernel,
        out_shape=exchange_shapes(rows),
        in_specs=vmem(SHIFTS + 2),
        out_specs=tuple(vmem(SHIFTS + 1)),
        compiler_params=pltpu.CompilerParams(vmem_limit_bytes=12 << 20),
        scratch_shapes=[
            pltpu.VMEM((wide, PATCH_CELLS), jnp.float32),
            pltpu.VMEM((members, LEVELS * PATCH_CELLS), jnp.bfloat16),
            pltpu.VMEM((LEVELS * PATCH_CELLS, slots), jnp.bfloat16),
        ],
        name="analysis",
    )(*in_vmem(*received, message))


def place_kernel(self_ref, got_ref, from_1, from_2, from_3, out_hbm, sem):
    member = lax.axis_index("member")
    row, core = member // 2, member % 2
    copies = []
    pieces = [self_ref, got_ref.at[0]]
    for ref in (from_1, from_2, from_3):
        pieces += [ref.at[0], ref.at[1]]
    for i, piece in enumerate(pieces):
        patch = (row + i // 2) % SHIFTS * 2 + (core + i) % 2
        lanes = pl.ds(pl.multiple_of(patch * PATCH_CELLS, PATCH_CELLS), PATCH_CELLS)
        copies.append(pltpu.make_async_copy(piece, out_hbm.at[:, lanes], sem.at[i]))
    for copy in copies:
        copy.start()
    for copy in copies:
        copy.wait()


def place(received, cells):
    rows = received[0].shape[0]
    return pl.pallas_call(
        place_kernel,
        out_shape=jax.ShapeDtypeStruct((rows, cells), jnp.bfloat16),
        in_specs=vmem(SHIFTS + 1),
        out_specs=pl.BlockSpec(memory_space=pltpu.HBM),
        scratch_shapes=[pltpu.SemaphoreType.DMA((2 * SHIFTS,))],
        compiler_params=pltpu.CompilerParams(vmem_limit_bytes=2 << 20),
        name="place",
    )(*in_vmem(*received))


def on_device(
    state, adjacent_columns, adjacent_rates, amplification_speed,
    obs_patch, obs_row, obs_value, obs_error,
):
    members, levels, cells = state.shape
    regions = lax.axis_size("region")
    groups = lax.axis_size("member")
    total = cells * regions
    flat = state.reshape(members * levels, cells)
    up_part, down_part, kept, coef, *observed = prepare(
        flat, adjacent_columns, adjacent_rates, amplification_speed[None, :],
        obs_patch[None, :], obs_row[None, :], obs_value[None, :], obs_error[None, :], total,
    )
    up = [(i, (i + 1) % regions) for i in range(regions)]
    left = lax.ppermute(up_part, "region", up)
    right = lax.ppermute(down_part, "region", [(j, i) for i, j in up])
    message = observation_message(*observed, regions, groups)
    message = lax.all_to_all(message, ("member", "region"), 0, 0, tiled=True)
    own = own_matrices(coef)
    parts = forecast(kept, left, right, own, coef)
    received = exchange(parts, 1)
    parts = analysis(received, message)
    back = exchange(parts, -1)
    return place(back, cells).reshape(members, levels, cells)


def solution(mesh):
    placed = (
        P("member", None, "region"),
        P(None, "region"),
        P(None, "region"),
        P("region"),
        P(("member", "region")),
        P(("member", "region")),
        P(("member", "region")),
        P(("member", "region")),
    )

    return jax.shard_map(
        on_device, mesh=mesh, in_specs=placed, out_specs=P("member", None, "region"), check_vma=False
    )
```

```python
import functools
import math

import jax
import jax.numpy as jnp
from jax import lax
from jax.experimental import pallas as pl
from jax.experimental.pallas import tpu as pltpu
from jax.sharding import PartitionSpec as P


PATCH_CELLS = 128
RIM = 256
STEPS = 3
NS_ITERS = 6
LEVELS = 8
BLOCK = 256
WINDOW = BLOCK + 2 * RIM
HALO = STEPS * RIM
COEF_ROWS = 16
TILE = 128
STATE_CHUNKS = 4
SHIFTS = 4
REST = (0, 1, 3)


def high(value):
    return value.astype(jnp.bfloat16)


def low(value):
    return (value - high(value).astype(jnp.float32)).astype(jnp.bfloat16)


def dot_f32(a, b, dims=(((1,), (0,)), ((), ()))):
    return lax.dot_general(a, b, dims, preferred_element_type=jnp.float32)


def dot_half(a, b, dims=(((1,), (0,)), ((), ()))):
    return dot_f32(high(a), high(b), dims)


def cell_offsets(columns, first, total):
    cell = first + lax.broadcasted_iota(jnp.int32, columns.shape, 1)
    offset = columns - cell
    offset = jnp.where(offset > total // 2, offset - total, offset)
    return jnp.where(offset < -(total // 2), offset + total, offset)


def matrix_tiles(matrix_ref, index, offsets, rates):
    offset = [offsets[k : k + 1] for k in range(6)]
    rate = [rates[k : k + 1] for k in range(6)]
    for k in range(6):
        for later in range(k + 1, 6):
            same = offset[later] == offset[k]
            rate[k] = rate[k] + jnp.where(same, rate[later], 0.0)
            offset[later] = jnp.where(same, float(-4 * RIM), offset[later])
    zero = jnp.zeros((TILE, TILE), jnp.bfloat16)
    row = lax.broadcasted_iota(jnp.int32, (TILE, TILE), 0).astype(jnp.float32)
    row = row.astype(jnp.bfloat16)
    lane = lax.broadcasted_iota(jnp.int32, (1, TILE), 1).astype(jnp.float32)
    reach = (TILE + 2 * RIM) // TILE
    steps = []
    for part in range(BLOCK // TILE):
        lanes = slice(part * TILE, (part + 1) * TILE)
        local = [item[:, lanes] + (lane + float(RIM)) for item in offset]
        spread = [item[:, lanes].astype(jnp.bfloat16) for item in rate]
        for tile in range(WINDOW // TILE):

            def write(tile=tile, part=part, lanes=lanes, local=local, spread=spread):
                rows = slice(tile * TILE, (tile + 1) * TILE)
                step = tile - part
                total = zero
                if 0 <= step < reach:
                    for k in range(6):
                        near = (local[k] - float(step * TILE)).astype(jnp.bfloat16)
                        hit = row == jnp.broadcast_to(near, (TILE, TILE))
                        total = jnp.where(hit, jnp.broadcast_to(spread[k], (TILE, TILE)), total)
                matrix_ref[index, rows, lanes] = total

            steps.append(write)
    return steps


def build_matrix(matrix_ref, index, offsets, rates):
    for step in matrix_tiles(matrix_ref, index, offsets, rates):
        step()


def fetches(sources, targets, sem):
    return [
        pltpu.make_async_copy(source, target, sem.at[i])
        for i, (source, target) in enumerate(zip(sources, targets))
    ]


def prepare_kernel(
    state_hbm, column_hbm, rate_hbm, speed_hbm, patch_hbm, row_hbm, value_hbm, error_hbm,
    up_ref, down_ref, state_ref, coef_ref, patch_ref, row_ref, value_ref, error_ref,
    column_ref, rate_ref, speed_ref, small_sem, later_sem, state_sem, *, total,
):
    rows, cells = state_ref.shape
    small = fetches(
        (column_hbm, rate_hbm, speed_hbm), (column_ref, rate_ref, speed_ref), small_sem
    )
    later = fetches(
        (patch_hbm, row_hbm, value_hbm, error_hbm),
        (patch_ref, row_ref, value_ref, error_ref),
        later_sem,
    )
    chunk = rows // STATE_CHUNKS
    large = [
        pltpu.make_async_copy(
            state_hbm.at[pl.ds(i * chunk, chunk)],
            state_ref.at[pl.ds(i * chunk, chunk)],
            state_sem.at[i],
        )
        for i in range(STATE_CHUNKS)
    ]
    for copy in small + large + later:
        copy.start()
    for copy in small:
        copy.wait()
    region = lax.axis_index("region")
    last = cells - HALO
    offsets = cell_offsets(column_ref[...], region * cells, total).astype(jnp.float32)
    rates = rate_ref[...]
    rate_sum = jnp.sum(rates, axis=0, keepdims=True)
    speed = speed_ref[...]
    coef_ref[...] = jnp.concatenate(
        [
            offsets,
            rates,
            high(rate_sum).astype(jnp.float32),
            low(rate_sum).astype(jnp.float32),
            high(speed).astype(jnp.float32),
            low(speed).astype(jnp.float32),
        ],
        axis=0,
    )
    up_ref[rows:] = coef_ref[:, last:].astype(jnp.bfloat16)
    down_ref[rows:] = coef_ref[:, :HALO].astype(jnp.bfloat16)
    for i, copy in enumerate(large):
        copy.wait()
        part = pl.ds(i * chunk, chunk)
        up_ref[part] = state_ref[part, last:].astype(jnp.bfloat16)
        down_ref[part] = state_ref[part, :HALO].astype(jnp.bfloat16)
    for copy in later:
        copy.wait()


def vmem(count):
    return [pl.BlockSpec(memory_space=pltpu.VMEM)] * count


def in_vmem(*values):
    return [pltpu.with_memory_space_constraint(value, pltpu.VMEM) for value in values]


def in_hbm(*values):
    return [pltpu.with_memory_space_constraint(value, pltpu.HBM) for value in values]


def prepare(state, columns, rates, speed, patch, row, value, error, total):
    rows, cells = state.shape
    side = pltpu.VMEM((rows + COEF_ROWS, HALO), jnp.bfloat16)
    return pl.pallas_call(
        functools.partial(prepare_kernel, total=total),
        out_shape=(
            side,
            side,
            pltpu.VMEM((rows, cells), jnp.float32),
            pltpu.VMEM((COEF_ROWS, cells), jnp.float32),
            *(pltpu.VMEM(item.shape, item.dtype) for item in (patch, row, value, error)),
        ),
        in_specs=[pl.BlockSpec(memory_space=pltpu.HBM)] * 8,
        out_specs=tuple(vmem(8)),
        scratch_shapes=[
            pltpu.VMEM(columns.shape, jnp.int32),
            pltpu.VMEM(rates.shape, jnp.float32),
            pltpu.VMEM(speed.shape, jnp.float32),
            pltpu.SemaphoreType.DMA((3,)),
            pltpu.SemaphoreType.DMA((4,)),
            pltpu.SemaphoreType.DMA((STATE_CHUNKS,)),
        ],
        compiler_params=pltpu.CompilerParams(vmem_limit_bytes=8 << 20),
        name="prepare",
    )(*in_hbm(state, columns, rates, speed, patch, row, value, error))


def matrices_kernel(coef_ref, matrix_ref):
    for b in range(matrix_ref.shape[0]):
        part = slice(b * BLOCK, (b + 1) * BLOCK)
        build_matrix(matrix_ref, b, coef_ref[0:6, part], coef_ref[6:12, part])


def own_matrices(coef):
    shape = (coef.shape[1] // BLOCK, WINDOW, BLOCK)
    return pl.pallas_call(
        matrices_kernel,
        out_shape=pltpu.VMEM(shape, jnp.bfloat16),
        in_specs=vmem(1),
        out_specs=vmem(1)[0],
        compiler_params=pltpu.CompilerParams(vmem_limit_bytes=4 << 20),
        name="own_matrices",
    )(*in_vmem(coef))


def message_kernel(patch_ref, row_ref, value_ref, error_ref, message_ref, *, regions, groups):
    devices, count = message_ref.shape[0], patch_ref.shape[1]
    target = lax.broadcasted_iota(jnp.int32, (devices, count), 0)
    wanted = target % regions * groups + target // regions
    hit = jnp.where(patch_ref[...] == wanted, 1.0, 0.0)
    before = lax.broadcasted_iota(jnp.int32, (count, count), 0)
    after = lax.broadcasted_iota(jnp.int32, (count, count), 1)
    earlier = jnp.where(before < after, 1.0, 0.0).astype(jnp.bfloat16)
    rank = dot_f32(hit.astype(jnp.bfloat16), earlier)
    field = lax.broadcasted_iota(jnp.int32, (message_ref.shape[1], count), 0)
    location = row_ref[...].astype(jnp.float32) + 1.0
    weight = 1.0 / (error_ref[...] * error_ref[...])
    message = None
    for slot in range(2):
        chosen = jnp.where(rank == float(slot), hit, 0.0).astype(jnp.bfloat16)
        values = jnp.zeros(field.shape, jnp.float32)
        for k, item in enumerate((location, value_ref[...], weight)):
            values = jnp.where(field == 3 * slot + k, item, values)
        for _ in range(3):
            piece = high(values)
            values = values - piece.astype(jnp.float32)
            term = dot_f32(chosen, piece, (((1,), (1,)), ((), ())))
            message = term if message is None else message + term
    message_ref[...] = message


def observation_message(patch, row, value, error, regions, groups):
    return pl.pallas_call(
        functools.partial(message_kernel, regions=regions, groups=groups),
        out_shape=jax.ShapeDtypeStruct((regions * groups, TILE), jnp.float32),
        in_specs=vmem(4),
        out_specs=vmem(1)[0],
        compiler_params=pltpu.CompilerParams(vmem_limit_bytes=4 << 20),
        name="message",
    )(*in_vmem(patch, row, value, error))


def forecast_kernel(
    state_ref, left_ref, right_ref, own_ref, own_coef_ref, own_0, own_1, own_2, own_3,
    first_swap, rest_swap, matrix_ref, coef_ref, field_a, field_b, wide_ref,
):
    rows, cells = state_ref.shape
    own_blocks = cells // BLOCK
    side_blocks = (STEPS - 1) * RIM // BLOCK
    blocks = own_blocks + 2 * side_blocks
    far = HALO + cells
    for ref, begin in ((left_ref, 0), (right_ref, far)):
        coef_ref[:, begin : begin + HALO] = ref[rows:].astype(jnp.float32)
        field_a[:, begin : begin + HALO] = ref[:rows]
    coef_ref[:, HALO:far] = own_coef_ref[...]
    field_a[:, HALO:far] = state_ref[...].astype(jnp.bfloat16)
    keep, speed, matrices = [], [], []
    for b in range(blocks):
        part = slice(RIM + b * BLOCK, RIM + (b + 1) * BLOCK)
        if side_blocks <= b < side_blocks + own_blocks:
            matrices.append((own_ref, b - side_blocks))
        else:
            index = b if b < side_blocks else b - own_blocks
            build_matrix(matrix_ref, index, coef_ref[0:6, part], coef_ref[6:12, part])
            matrices.append((matrix_ref, index))
        keep.append(1.0 - (coef_ref[12:13, part] + coef_ref[13:14, part]))
        speed.append(coef_ref[14:15, part] + coef_ref[15:16, part])
    source, target = field_a, field_b
    for step in range(STEPS - 1):
        for b in range(step, blocks - step):
            first = b * BLOCK
            middle = slice(first + RIM, first + RIM + BLOCK)
            holder, index = matrices[b]
            summed = dot_f32(source[:, first : first + WINDOW], holder[index])
            if step > 0:
                centre = wide_ref[:, middle]
            elif side_blocks <= b < side_blocks + own_blocks:
                own = (b - side_blocks) * BLOCK
                centre = state_ref[:, own : own + BLOCK]
            else:
                centre = source[:, middle].astype(jnp.float32)
            blended = centre * keep[b] + summed
            result = blended + speed[b] * jnp.tanh(blended)
            wide_ref[:, middle] = result
            target[:, middle] = result.astype(jnp.bfloat16)
        source, target = target, source
    member = lax.axis_index("member")
    row, core = member // 2, member % 2
    for shift, own_out in enumerate((own_0, own_1, own_2, own_3)):
        block = (row + shift) % own_blocks
        first = pl.multiple_of(block * BLOCK + (HALO - RIM), TILE)
        middle = pl.ds(pl.multiple_of(block * BLOCK + HALO, TILE), BLOCK)
        summed = dot_f32(source[:, pl.ds(first, WINDOW)], own_ref[block])
        kept = 1.0 - (coef_ref[12:13, middle] + coef_ref[13:14, middle])
        quick = coef_ref[14:15, middle] + coef_ref[15:16, middle]
        blended = wide_ref[:, middle] * kept + summed
        result = (blended + quick * jnp.tanh(blended)).astype(jnp.bfloat16)
        even, odd_half = result[:, :PATCH_CELLS], result[:, PATCH_CELLS:]
        own_out[...] = jnp.where(core == 0, even, odd_half)
        store_swap(shift, jnp.where(core == 0, odd_half, even), first_swap, rest_swap)


def exchange_shapes(rows):
    return (pltpu.VMEM((rows, PATCH_CELLS), jnp.bfloat16),) * (SHIFTS + 1) + (
        pltpu.VMEM((len(REST), rows, PATCH_CELLS), jnp.bfloat16),
    )


def store_swap(shift, value, first_ref, rest_ref):
    if shift in REST:
        rest_ref[REST.index(shift)] = value
    else:
        first_ref[...] = value


def forecast(state, left, right, own, coef):
    rows, cells = state.shape
    sides = 2 * (STEPS - 1) * RIM // BLOCK
    padded = cells + 2 * HALO
    return pl.pallas_call(
        forecast_kernel,
        out_shape=exchange_shapes(rows),
        in_specs=vmem(5),
        out_specs=tuple(vmem(SHIFTS + 2)),
        scratch_shapes=[
            pltpu.VMEM((sides, WINDOW, BLOCK), jnp.bfloat16),
            pltpu.VMEM((COEF_ROWS, padded), jnp.float32),
            pltpu.VMEM((rows, padded), jnp.bfloat16),
            pltpu.VMEM((rows, padded), jnp.bfloat16),
            pltpu.VMEM((rows, padded), jnp.float32),
        ],
        compiler_params=pltpu.CompilerParams(vmem_limit_bytes=16 << 20),
        name="forecast",
    )(*in_vmem(state, left, right, own, coef))


def merge_kernel(own_2, got_ref, out_2):
    out_2[0] = own_2[...]
    out_2[1] = got_ref[...]


def merge_rest_kernel(own_1, own_3, got_ref, out_1, out_3):
    for shift, own, out in ((1, own_1, out_1), (3, own_3, out_3)):
        out[0] = own[...]
        out[1] = got_ref[REST.index(shift)]


def merge(kernel, *parts):
    rows = parts[0].shape[0]
    count = len(parts) - 1
    return pl.pallas_call(
        kernel,
        out_shape=(pltpu.VMEM((2, rows, PATCH_CELLS), jnp.bfloat16),) * count,
        in_specs=vmem(count + 1),
        out_specs=tuple(vmem(count)),
        compiler_params=pltpu.CompilerParams(vmem_limit_bytes=2 << 20),
    )(*in_vmem(*parts))


def exchange(parts, sign):
    groups = lax.axis_size("member")
    swap = [(i, i ^ 1) for i in range(groups)]
    *own, first_swap, rest_swap = parts
    got_first = lax.ppermute(first_swap, "member", swap)
    got_rest = lax.ppermute(rest_swap, "member", swap)
    (merged_2,) = merge(merge_kernel, own[2], got_first)
    merged_1, merged_3 = merge(merge_rest_kernel, own[1], own[3], got_rest)
    moved = {}
    for shift, merged in ((2, merged_2), (1, merged_1), (3, merged_3)):
        edges = [(i, (i + sign * 2 * shift) % groups) for i in range(groups)]
        moved[shift] = lax.ppermute(merged, "member", edges)
    return own[0], got_rest, moved[1], moved[2], moved[3]


def analysis_kernel(
    self_ref, got_ref, from_1, from_2, from_3, message_ref, own_0, own_1, own_2, own_3,
    first_swap, rest_swap, wide_ref, x2_ref, select_ref,
):
    rows = self_ref.shape[0]
    members = wide_ref.shape[0] // LEVELS
    span = LEVELS * PATCH_CELLS
    arrived = [self_ref[...], got_ref[0]]
    for ref in (from_1, from_2, from_3):
        arrived += [ref[0], ref[1]]
    for i, piece in enumerate(arrived):
        wide_ref[i * rows : (i + 1) * rows] = piece.astype(jnp.float32)
    for level in range(LEVELS):
        part = wide_ref[pl.ds(level, members, stride=LEVELS), :]
        x2_ref[:, level * PATCH_CELLS : (level + 1) * PATCH_CELLS] = part.astype(jnp.bfloat16)
    message = jnp.transpose(message_ref[...])
    location = jnp.concatenate([message[0:1], message[3:4]], axis=1) - 1.0
    value = jnp.concatenate([message[1:2], message[4:5]], axis=1)
    weight = jnp.concatenate([message[2:3], message[5:6]], axis=1)
    slots = location.shape[1]
    location = location.astype(jnp.int32)
    for first in range(0, span, PATCH_CELLS):
        row = lax.broadcasted_iota(jnp.int32, (PATCH_CELLS, slots), 0) + first
        hot = jnp.where(row == location, 1.0, 0.0)
        select_ref[first : first + PATCH_CELLS, :] = hot.astype(jnp.bfloat16)
    seen = dot_f32(x2_ref[...], select_ref[...])
    seen_mean = jnp.sum(seen, axis=0, keepdims=True) * (1.0 / members)
    rooted = jnp.sqrt(weight)
    spread = 1.0 / math.sqrt(members - 1.0)
    scaled = (seen - seen_mean) * (rooted * spread)
    row = lax.broadcasted_iota(jnp.int32, (members, members), 0)
    column = lax.broadcasted_iota(jnp.int32, (members, members), 1)
    diagonal = jnp.where(row == column, 1.0, 0.0)
    product = dot_half(scaled, scaled, (((1,), (1,)), ((), ())))
    system = diagonal + product
    square = jnp.sum(jnp.sum(system * system, axis=0, keepdims=True), axis=1, keepdims=True)
    inverse_scale = jnp.broadcast_to(lax.rsqrt(square), (1, members))
    innovation = rooted * (value - seen_mean) * spread
    forcing = jnp.sum(scaled * innovation, axis=1, keepdims=True)
    p, z = inverse_scale, jnp.ones_like(inverse_scale)
    both = product * inverse_scale
    root = None
    for sweep in range(NS_ITERS):
        f = 1.5 - 0.5 * p
        factor = -0.5 * both
        narrow = factor.astype(jnp.bfloat16)
        if root is None:
            new_root = factor
        else:
            new_root = z * factor + f * root
        if sweep < NS_ITERS - 1:
            once = p * factor + f * both
            if root is None:
                once = once + dot_f32(high(both), narrow)
            else:
                stacked = dot_f32(jnp.concatenate([high(both), high(root)], axis=0), narrow)
                once = once + stacked[:members]
                new_root = new_root + stacked[members:]
            q = p * f
            both = q * factor + f * once + dot_f32(high(once), narrow)
            p = q * f
        else:
            new_root = new_root + dot_f32(high(root), narrow)
        root, z = new_root, z * f
    whole = root + z * diagonal
    inner = jnp.sum(whole * forcing, axis=0, keepdims=True)
    shift = jnp.sum(whole * inner, axis=1, keepdims=True) * inverse_scale[:, 0:1]
    half_scale = jnp.sqrt(inverse_scale)
    transform = (root * half_scale).astype(jnp.bfloat16)
    direct = (z * half_scale)[:, 0:PATCH_CELLS]
    pair = 2
    for level in range(0, LEVELS, pair):
        pieces = []
        for k in range(level, level + pair):
            part = x2_ref[:, k * PATCH_CELLS : (k + 1) * PATCH_CELLS].astype(jnp.float32)
            mean = jnp.sum(part, axis=0, keepdims=True) * (1.0 / members)
            anomaly = part - mean
            base = mean + jnp.sum(anomaly * shift, axis=0, keepdims=True) + direct * anomaly
            pieces.append((anomaly.astype(jnp.bfloat16), base))
        moved = dot_f32(transform, jnp.concatenate([piece[0] for piece in pieces], axis=1))
        for k in range(pair):
            updated = pieces[k][1] + moved[:, k * PATCH_CELLS : (k + 1) * PATCH_CELLS]
            wide_ref[pl.ds(level + k, members, stride=LEVELS), :] = updated
    for shift, own in enumerate((own_0, own_1, own_2, own_3)):
        first = 2 * shift * rows
        own[...] = wide_ref[first : first + rows].astype(jnp.bfloat16)
        other = wide_ref[first + rows : first + 2 * rows].astype(jnp.bfloat16)
        store_swap(shift, other, first_swap, rest_swap)


def analysis(received, message):
    rows = received[0].shape[0]
    wide = 2 * SHIFTS * rows
    members = wide // LEVELS
    slots = 2 * message.shape[0]
    return pl.pallas_call(
        analysis_kernel,
        out_shape=exchange_shapes(rows),
        in_specs=vmem(SHIFTS + 2),
        out_specs=tuple(vmem(SHIFTS + 2)),
        compiler_params=pltpu.CompilerParams(vmem_limit_bytes=12 << 20),
        scratch_shapes=[
            pltpu.VMEM((wide, PATCH_CELLS), jnp.float32),
            pltpu.VMEM((members, LEVELS * PATCH_CELLS), jnp.bfloat16),
            pltpu.VMEM((LEVELS * PATCH_CELLS, slots), jnp.bfloat16),
        ],
        name="analysis",
    )(*in_vmem(*received, message))


def place_kernel(self_ref, got_ref, from_1, from_2, from_3, out_hbm, sem):
    member = lax.axis_index("member")
    row, core = member // 2, member % 2
    copies = []
    pieces = [self_ref, got_ref.at[0]]
    for ref in (from_1, from_2, from_3):
        pieces += [ref.at[0], ref.at[1]]
    for i, piece in enumerate(pieces):
        patch = (row + i // 2) % SHIFTS * 2 + (core + i) % 2
        lanes = pl.ds(pl.multiple_of(patch * PATCH_CELLS, PATCH_CELLS), PATCH_CELLS)
        copies.append(pltpu.make_async_copy(piece, out_hbm.at[:, lanes], sem.at[i]))
    for copy in copies:
        copy.start()
    for copy in copies:
        copy.wait()


def place(received, cells):
    rows = received[0].shape[0]
    return pl.pallas_call(
        place_kernel,
        out_shape=jax.ShapeDtypeStruct((rows, cells), jnp.bfloat16),
        in_specs=vmem(SHIFTS + 1),
        out_specs=pl.BlockSpec(memory_space=pltpu.HBM),
        scratch_shapes=[pltpu.SemaphoreType.DMA((2 * SHIFTS,))],
        compiler_params=pltpu.CompilerParams(vmem_limit_bytes=2 << 20),
        name="place",
    )(*in_vmem(*received))


def on_device(
    state, adjacent_columns, adjacent_rates, amplification_speed,
    obs_patch, obs_row, obs_value, obs_error,
):
    members, levels, cells = state.shape
    regions = lax.axis_size("region")
    groups = lax.axis_size("member")
    total = cells * regions
    flat = state.reshape(members * levels, cells)
    up_part, down_part, kept, coef, *observed = prepare(
        flat, adjacent_columns, adjacent_rates, amplification_speed[None, :],
        obs_patch[None, :], obs_row[None, :], obs_value[None, :], obs_error[None, :], total,
    )
    up = [(i, (i + 1) % regions) for i in range(regions)]
    left = lax.ppermute(up_part, "region", up)
    right = lax.ppermute(down_part, "region", [(j, i) for i, j in up])
    message = observation_message(*observed, regions, groups)
    message = lax.all_to_all(message, ("member", "region"), 0, 0, tiled=True)
    own = own_matrices(coef)
    parts = forecast(kept, left, right, own, coef)
    received = exchange(parts, 1)
    parts = analysis(received, message)
    back = exchange(parts, -1)
    return place(back, cells).reshape(members, levels, cells)


def solution(mesh):
    placed = (
        P("member", None, "region"),
        P(None, "region"),
        P(None, "region"),
        P("region"),
        P(("member", "region")),
        P(("member", "region")),
        P(("member", "region")),
        P(("member", "region")),
    )

    return jax.shard_map(
        on_device, mesh=mesh, in_specs=placed, out_specs=P("member", None, "region"), check_vma=False
    )
```

```python
import functools
import math

import jax
import jax.numpy as jnp
from jax import lax
from jax.experimental import pallas as pl
from jax.experimental.pallas import tpu as pltpu
from jax.sharding import PartitionSpec as P


PATCH_CELLS = 128
RIM = 256
STEPS = 3
NS_ITERS = 6
LEVELS = 8
BLOCK = 256
WINDOW = BLOCK + 2 * RIM
HALO = STEPS * RIM
COEF_ROWS = 16
TILE = 128
STATE_CHUNKS = 4
SHIFTS = 4
REST = (0, 1, 3)


def high(value):
    return value.astype(jnp.bfloat16)


def low(value):
    return (value - high(value).astype(jnp.float32)).astype(jnp.bfloat16)


def dot_f32(a, b, dims=(((1,), (0,)), ((), ()))):
    return lax.dot_general(a, b, dims, preferred_element_type=jnp.float32)


def dot_half(a, b, dims=(((1,), (0,)), ((), ()))):
    return dot_f32(high(a), high(b), dims)


def cell_offsets(columns, first, total):
    cell = first + lax.broadcasted_iota(jnp.int32, columns.shape, 1)
    offset = columns - cell
    offset = jnp.where(offset > total // 2, offset - total, offset)
    return jnp.where(offset < -(total // 2), offset + total, offset)


def matrix_tiles(matrix_ref, index, offsets, rates):
    offset = [offsets[k : k + 1] for k in range(6)]
    rate = [rates[k : k + 1] for k in range(6)]
    for k in range(6):
        for later in range(k + 1, 6):
            same = offset[later] == offset[k]
            rate[k] = rate[k] + jnp.where(same, rate[later], 0.0)
            offset[later] = jnp.where(same, float(-4 * RIM), offset[later])
    zero = jnp.zeros((TILE, TILE), jnp.bfloat16)
    row = lax.broadcasted_iota(jnp.int32, (TILE, TILE), 0).astype(jnp.float32)
    row = row.astype(jnp.bfloat16)
    lane = lax.broadcasted_iota(jnp.int32, (1, TILE), 1).astype(jnp.float32)
    reach = (TILE + 2 * RIM) // TILE
    steps = []
    for part in range(BLOCK // TILE):
        lanes = slice(part * TILE, (part + 1) * TILE)
        local = [item[:, lanes] + (lane + float(RIM)) for item in offset]
        spread = [item[:, lanes].astype(jnp.bfloat16) for item in rate]
        for tile in range(WINDOW // TILE):

            def write(tile=tile, part=part, lanes=lanes, local=local, spread=spread):
                rows = slice(tile * TILE, (tile + 1) * TILE)
                step = tile - part
                total = zero
                if 0 <= step < reach:
                    for k in range(6):
                        near = (local[k] - float(step * TILE)).astype(jnp.bfloat16)
                        hit = row == jnp.broadcast_to(near, (TILE, TILE))
                        total = jnp.where(hit, jnp.broadcast_to(spread[k], (TILE, TILE)), total)
                matrix_ref[index, rows, lanes] = total

            steps.append(write)
    return steps


def build_matrix(matrix_ref, index, offsets, rates):
    for step in matrix_tiles(matrix_ref, index, offsets, rates):
        step()


def fetches(sources, targets, sem):
    return [
        pltpu.make_async_copy(source, target, sem.at[i])
        for i, (source, target) in enumerate(zip(sources, targets))
    ]


def prepare_kernel(
    state_hbm, column_hbm, rate_hbm, speed_hbm, patch_hbm, row_hbm, value_hbm, error_hbm,
    up_ref, down_ref, state_ref, coef_ref, patch_ref, row_ref, value_ref, error_ref,
    column_ref, rate_ref, speed_ref, small_sem, later_sem, state_sem, *, total,
):
    rows, cells = state_ref.shape
    small = fetches(
        (column_hbm, rate_hbm, speed_hbm), (column_ref, rate_ref, speed_ref), small_sem
    )
    later = fetches(
        (patch_hbm, row_hbm, value_hbm, error_hbm),
        (patch_ref, row_ref, value_ref, error_ref),
        later_sem,
    )
    chunk = rows // STATE_CHUNKS
    large = [
        pltpu.make_async_copy(
            state_hbm.at[pl.ds(i * chunk, chunk)],
            state_ref.at[pl.ds(i * chunk, chunk)],
            state_sem.at[i],
        )
        for i in range(STATE_CHUNKS)
    ]
    for copy in small + large + later:
        copy.start()
    for copy in small:
        copy.wait()
    region = lax.axis_index("region")
    last = cells - HALO
    offsets = cell_offsets(column_ref[...], region * cells, total).astype(jnp.float32)
    rates = rate_ref[...]
    rate_sum = jnp.sum(rates, axis=0, keepdims=True)
    speed = speed_ref[...]
    coef_ref[...] = jnp.concatenate(
        [
            offsets,
            rates,
            high(rate_sum).astype(jnp.float32),
            low(rate_sum).astype(jnp.float32),
            high(speed).astype(jnp.float32),
            low(speed).astype(jnp.float32),
        ],
        axis=0,
    )
    up_ref[rows:] = coef_ref[:, last:].astype(jnp.bfloat16)
    down_ref[rows:] = coef_ref[:, :HALO].astype(jnp.bfloat16)
    for i, copy in enumerate(large):
        copy.wait()
        part = pl.ds(i * chunk, chunk)
        up_ref[part] = state_ref[part, last:].astype(jnp.bfloat16)
        down_ref[part] = state_ref[part, :HALO].astype(jnp.bfloat16)
    for copy in later:
        copy.wait()


def vmem(count):
    return [pl.BlockSpec(memory_space=pltpu.VMEM)] * count


def in_vmem(*values):
    return [pltpu.with_memory_space_constraint(value, pltpu.VMEM) for value in values]


def in_hbm(*values):
    return [pltpu.with_memory_space_constraint(value, pltpu.HBM) for value in values]


def prepare(state, columns, rates, speed, patch, row, value, error, total):
    rows, cells = state.shape
    side = pltpu.VMEM((rows + COEF_ROWS, HALO), jnp.bfloat16)
    return pl.pallas_call(
        functools.partial(prepare_kernel, total=total),
        out_shape=(
            side,
            side,
            pltpu.VMEM((rows, cells), jnp.float32),
            pltpu.VMEM((COEF_ROWS, cells), jnp.float32),
            *(pltpu.VMEM(item.shape, item.dtype) for item in (patch, row, value, error)),
        ),
        in_specs=[pl.BlockSpec(memory_space=pltpu.HBM)] * 8,
        out_specs=tuple(vmem(8)),
        scratch_shapes=[
            pltpu.VMEM(columns.shape, jnp.int32),
            pltpu.VMEM(rates.shape, jnp.float32),
            pltpu.VMEM(speed.shape, jnp.float32),
            pltpu.SemaphoreType.DMA((3,)),
            pltpu.SemaphoreType.DMA((4,)),
            pltpu.SemaphoreType.DMA((STATE_CHUNKS,)),
        ],
        compiler_params=pltpu.CompilerParams(vmem_limit_bytes=8 << 20),
        name="prepare",
    )(*in_hbm(state, columns, rates, speed, patch, row, value, error))


def matrices_kernel(coef_ref, matrix_ref):
    for b in range(matrix_ref.shape[0]):
        part = slice(b * BLOCK, (b + 1) * BLOCK)
        build_matrix(matrix_ref, b, coef_ref[0:6, part], coef_ref[6:12, part])


def own_matrices(coef):
    shape = (coef.shape[1] // BLOCK, WINDOW, BLOCK)
    return pl.pallas_call(
        matrices_kernel,
        out_shape=pltpu.VMEM(shape, jnp.bfloat16),
        in_specs=vmem(1),
        out_specs=vmem(1)[0],
        compiler_params=pltpu.CompilerParams(vmem_limit_bytes=4 << 20),
        name="own_matrices",
    )(*in_vmem(coef))


def right_kernel(right_ref, matrix_ref):
    rows = right_ref.shape[0] - COEF_ROWS
    for b in range(matrix_ref.shape[0]):
        part = slice(b * BLOCK, (b + 1) * BLOCK)
        coef = right_ref[rows:, part].astype(jnp.float32)
        build_matrix(matrix_ref, b, coef[0:6], coef[6:12])


def right_matrices(right):
    shape = ((STEPS - 1) * RIM // BLOCK, WINDOW, BLOCK)
    return pl.pallas_call(
        right_kernel,
        out_shape=pltpu.VMEM(shape, jnp.bfloat16),
        in_specs=vmem(1),
        out_specs=vmem(1)[0],
        compiler_params=pltpu.CompilerParams(vmem_limit_bytes=3 << 20),
        name="right_matrices",
    )(*in_vmem(right))


def message_kernel(patch_ref, row_ref, value_ref, error_ref, message_ref, *, regions, groups):
    devices, count = message_ref.shape[0], patch_ref.shape[1]
    target = lax.broadcasted_iota(jnp.int32, (devices, count), 0)
    wanted = target % regions * groups + target // regions
    hit = jnp.where(patch_ref[...] == wanted, 1.0, 0.0)
    before = lax.broadcasted_iota(jnp.int32, (count, count), 0)
    after = lax.broadcasted_iota(jnp.int32, (count, count), 1)
    earlier = jnp.where(before < after, 1.0, 0.0).astype(jnp.bfloat16)
    rank = dot_f32(hit.astype(jnp.bfloat16), earlier)
    field = lax.broadcasted_iota(jnp.int32, (message_ref.shape[1], count), 0)
    location = row_ref[...].astype(jnp.float32) + 1.0
    weight = 1.0 / (error_ref[...] * error_ref[...])
    message = None
    for slot in range(2):
        chosen = jnp.where(rank == float(slot), hit, 0.0).astype(jnp.bfloat16)
        values = jnp.zeros(field.shape, jnp.float32)
        for k, item in enumerate((location, value_ref[...], weight)):
            values = jnp.where(field == 3 * slot + k, item, values)
        for _ in range(3):
            piece = high(values)
            values = values - piece.astype(jnp.float32)
            term = dot_f32(chosen, piece, (((1,), (1,)), ((), ())))
            message = term if message is None else message + term
    message_ref[...] = message


def observation_message(patch, row, value, error, regions, groups):
    return pl.pallas_call(
        functools.partial(message_kernel, regions=regions, groups=groups),
        out_shape=jax.ShapeDtypeStruct((regions * groups, TILE), jnp.float32),
        in_specs=vmem(4),
        out_specs=vmem(1)[0],
        compiler_params=pltpu.CompilerParams(vmem_limit_bytes=4 << 20),
        name="message",
    )(*in_vmem(patch, row, value, error))


def forecast_kernel(
    state_ref, left_ref, right_ref, own_ref, side_ref, own_coef_ref, own_0, own_1, own_2, own_3,
    first_swap, rest_swap, matrix_ref, coef_ref, field_a, field_b, wide_ref,
):
    rows, cells = state_ref.shape
    own_blocks = cells // BLOCK
    side_blocks = (STEPS - 1) * RIM // BLOCK
    blocks = own_blocks + 2 * side_blocks
    far = HALO + cells
    for ref, begin in ((left_ref, 0), (right_ref, far)):
        coef_ref[:, begin : begin + HALO] = ref[rows:].astype(jnp.float32)
        field_a[:, begin : begin + HALO] = ref[:rows]
    coef_ref[:, HALO:far] = own_coef_ref[...]
    field_a[:, HALO:far] = state_ref[...].astype(jnp.bfloat16)
    keep, speed, matrices = [], [], []
    for b in range(blocks):
        part = slice(RIM + b * BLOCK, RIM + (b + 1) * BLOCK)
        if b >= side_blocks + own_blocks:
            matrices.append((side_ref, b - side_blocks - own_blocks))
        elif b >= side_blocks:
            matrices.append((own_ref, b - side_blocks))
        else:
            build_matrix(matrix_ref, b, coef_ref[0:6, part], coef_ref[6:12, part])
            matrices.append((matrix_ref, b))
        keep.append(1.0 - (coef_ref[12:13, part] + coef_ref[13:14, part]))
        speed.append(coef_ref[14:15, part] + coef_ref[15:16, part])
    source, target = field_a, field_b
    for step in range(STEPS - 1):
        for b in range(step, blocks - step):
            first = b * BLOCK
            middle = slice(first + RIM, first + RIM + BLOCK)
            holder, index = matrices[b]
            summed = dot_f32(source[:, first : first + WINDOW], holder[index])
            if step > 0:
                centre = wide_ref[:, middle]
            elif side_blocks <= b < side_blocks + own_blocks:
                own = (b - side_blocks) * BLOCK
                centre = state_ref[:, own : own + BLOCK]
            else:
                centre = source[:, middle].astype(jnp.float32)
            blended = centre * keep[b] + summed
            result = blended + speed[b] * jnp.tanh(blended)
            wide_ref[:, middle] = result
            target[:, middle] = result.astype(jnp.bfloat16)
        source, target = target, source
    member = lax.axis_index("member")
    row, core = member // 2, member % 2
    for shift, own_out in enumerate((own_0, own_1, own_2, own_3)):
        block = (row + shift) % own_blocks
        first = pl.multiple_of(block * BLOCK + (HALO - RIM), TILE)
        middle = pl.ds(pl.multiple_of(block * BLOCK + HALO, TILE), BLOCK)
        summed = dot_f32(source[:, pl.ds(first, WINDOW)], own_ref[block])
        kept = 1.0 - (coef_ref[12:13, middle] + coef_ref[13:14, middle])
        quick = coef_ref[14:15, middle] + coef_ref[15:16, middle]
        blended = wide_ref[:, middle] * kept + summed
        result = (blended + quick * jnp.tanh(blended)).astype(jnp.bfloat16)
        even, odd_half = result[:, :PATCH_CELLS], result[:, PATCH_CELLS:]
        own_out[...] = jnp.where(core == 0, even, odd_half)
        store_swap(shift, jnp.where(core == 0, odd_half, even), first_swap, rest_swap)


def exchange_shapes(rows):
    return (pltpu.VMEM((rows, PATCH_CELLS), jnp.bfloat16),) * (SHIFTS + 1) + (
        pltpu.VMEM((len(REST), rows, PATCH_CELLS), jnp.bfloat16),
    )


def store_swap(shift, value, first_ref, rest_ref):
    if shift in REST:
        rest_ref[REST.index(shift)] = value
    else:
        first_ref[...] = value


def forecast(state, left, right, own, side, coef):
    rows, cells = state.shape
    sides = (STEPS - 1) * RIM // BLOCK
    padded = cells + 2 * HALO
    return pl.pallas_call(
        forecast_kernel,
        out_shape=exchange_shapes(rows),
        in_specs=vmem(6),
        out_specs=tuple(vmem(SHIFTS + 2)),
        scratch_shapes=[
            pltpu.VMEM((sides, WINDOW, BLOCK), jnp.bfloat16),
            pltpu.VMEM((COEF_ROWS, padded), jnp.float32),
            pltpu.VMEM((rows, padded), jnp.bfloat16),
            pltpu.VMEM((rows, padded), jnp.bfloat16),
            pltpu.VMEM((rows, padded), jnp.float32),
        ],
        compiler_params=pltpu.CompilerParams(vmem_limit_bytes=16 << 20),
        name="forecast",
    )(*in_vmem(state, left, right, own, side, coef))


def merge_kernel(own_2, got_ref, out_2):
    out_2[0] = own_2[...]
    out_2[1] = got_ref[...]


def merge_rest_kernel(own_1, own_3, got_ref, out_1, out_3):
    for shift, own, out in ((1, own_1, out_1), (3, own_3, out_3)):
        out[0] = own[...]
        out[1] = got_ref[REST.index(shift)]


def merge(kernel, *parts):
    rows = parts[0].shape[0]
    count = len(parts) - 1
    return pl.pallas_call(
        kernel,
        out_shape=(pltpu.VMEM((2, rows, PATCH_CELLS), jnp.bfloat16),) * count,
        in_specs=vmem(count + 1),
        out_specs=tuple(vmem(count)),
        compiler_params=pltpu.CompilerParams(vmem_limit_bytes=2 << 20),
    )(*in_vmem(*parts))


def exchange(parts, sign):
    groups = lax.axis_size("member")
    swap = [(i, i ^ 1) for i in range(groups)]
    *own, first_swap, rest_swap = parts
    got_first = lax.ppermute(first_swap, "member", swap)
    got_rest = lax.ppermute(rest_swap, "member", swap)
    (merged_2,) = merge(merge_kernel, own[2], got_first)
    merged_1, merged_3 = merge(merge_rest_kernel, own[1], own[3], got_rest)
    moved = {}
    for shift, merged in ((2, merged_2), (1, merged_1), (3, merged_3)):
        edges = [(i, (i + sign * 2 * shift) % groups) for i in range(groups)]
        moved[shift] = lax.ppermute(merged, "member", edges)
    return own[0], got_rest, moved[1], moved[2], moved[3]


def analysis_kernel(
    self_ref, got_ref, from_1, from_2, from_3, message_ref, own_0, own_1, own_2, own_3,
    first_swap, rest_swap, wide_ref, x2_ref, select_ref,
):
    rows = self_ref.shape[0]
    members = wide_ref.shape[0] // LEVELS
    span = LEVELS * PATCH_CELLS
    arrived = [self_ref[...], got_ref[0]]
    for ref in (from_1, from_2, from_3):
        arrived += [ref[0], ref[1]]
    for i, piece in enumerate(arrived):
        wide_ref[i * rows : (i + 1) * rows] = piece.astype(jnp.float32)
    for level in range(LEVELS):
        part = wide_ref[pl.ds(level, members, stride=LEVELS), :]
        x2_ref[:, level * PATCH_CELLS : (level + 1) * PATCH_CELLS] = part.astype(jnp.bfloat16)
    message = jnp.transpose(message_ref[...])
    location = jnp.concatenate([message[0:1], message[3:4]], axis=1) - 1.0
    value = jnp.concatenate([message[1:2], message[4:5]], axis=1)
    weight = jnp.concatenate([message[2:3], message[5:6]], axis=1)
    slots = location.shape[1]
    location = location.astype(jnp.int32)
    for first in range(0, span, PATCH_CELLS):
        row = lax.broadcasted_iota(jnp.int32, (PATCH_CELLS, slots), 0) + first
        hot = jnp.where(row == location, 1.0, 0.0)
        select_ref[first : first + PATCH_CELLS, :] = hot.astype(jnp.bfloat16)
    seen = dot_f32(x2_ref[...], select_ref[...])
    seen_mean = jnp.sum(seen, axis=0, keepdims=True) * (1.0 / members)
    rooted = jnp.sqrt(weight)
    spread = 1.0 / math.sqrt(members - 1.0)
    scaled = (seen - seen_mean) * (rooted * spread)
    row = lax.broadcasted_iota(jnp.int32, (members, members), 0)
    column = lax.broadcasted_iota(jnp.int32, (members, members), 1)
    diagonal = jnp.where(row == column, 1.0, 0.0)
    product = dot_half(scaled, scaled, (((1,), (1,)), ((), ())))
    system = diagonal + product
    square = jnp.sum(jnp.sum(system * system, axis=0, keepdims=True), axis=1, keepdims=True)
    inverse_scale = jnp.broadcast_to(lax.rsqrt(square), (1, members))
    innovation = rooted * (value - seen_mean) * spread
    forcing = jnp.sum(scaled * innovation, axis=1, keepdims=True)
    p, z = inverse_scale, jnp.ones_like(inverse_scale)
    both = product * inverse_scale
    root = None
    for sweep in range(NS_ITERS):
        f = 1.5 - 0.5 * p
        factor = -0.5 * both
        narrow = factor.astype(jnp.bfloat16)
        if root is None:
            new_root = factor
        else:
            new_root = z * factor + f * root
        if sweep < NS_ITERS - 1:
            once = p * factor + f * both
            if root is None:
                once = once + dot_f32(high(both), narrow)
            else:
                stacked = dot_f32(jnp.concatenate([high(both), high(root)], axis=0), narrow)
                once = once + stacked[:members]
                new_root = new_root + stacked[members:]
            q = p * f
            both = q * factor + f * once + dot_f32(high(once), narrow)
            p = q * f
        else:
            new_root = new_root + dot_f32(high(root), narrow)
        root, z = new_root, z * f
    whole = root + z * diagonal
    inner = jnp.sum(whole * forcing, axis=0, keepdims=True)
    shift = jnp.sum(whole * inner, axis=1, keepdims=True) * inverse_scale[:, 0:1]
    half_scale = jnp.sqrt(inverse_scale)
    transform = (root * half_scale).astype(jnp.bfloat16)
    direct = (z * half_scale)[:, 0:PATCH_CELLS]
    pair = 2
    for level in range(0, LEVELS, pair):
        pieces = []
        for k in range(level, level + pair):
            part = x2_ref[:, k * PATCH_CELLS : (k + 1) * PATCH_CELLS].astype(jnp.float32)
            mean = jnp.sum(part, axis=0, keepdims=True) * (1.0 / members)
            anomaly = part - mean
            base = mean + jnp.sum(anomaly * shift, axis=0, keepdims=True) + direct * anomaly
            pieces.append((anomaly.astype(jnp.bfloat16), base))
        moved = dot_f32(transform, jnp.concatenate([piece[0] for piece in pieces], axis=1))
        for k in range(pair):
            updated = pieces[k][1] + moved[:, k * PATCH_CELLS : (k + 1) * PATCH_CELLS]
            wide_ref[pl.ds(level + k, members, stride=LEVELS), :] = updated
    for shift, own in enumerate((own_0, own_1, own_2, own_3)):
        first = 2 * shift * rows
        own[...] = wide_ref[first : first + rows].astype(jnp.bfloat16)
        other = wide_ref[first + rows : first + 2 * rows].astype(jnp.bfloat16)
        store_swap(shift, other, first_swap, rest_swap)


def analysis(received, message):
    rows = received[0].shape[0]
    wide = 2 * SHIFTS * rows
    members = wide // LEVELS
    slots = 2 * message.shape[0]
    return pl.pallas_call(
        analysis_kernel,
        out_shape=exchange_shapes(rows),
        in_specs=vmem(SHIFTS + 2),
        out_specs=tuple(vmem(SHIFTS + 2)),
        compiler_params=pltpu.CompilerParams(vmem_limit_bytes=12 << 20),
        scratch_shapes=[
            pltpu.VMEM((wide, PATCH_CELLS), jnp.float32),
            pltpu.VMEM((members, LEVELS * PATCH_CELLS), jnp.bfloat16),
            pltpu.VMEM((LEVELS * PATCH_CELLS, slots), jnp.bfloat16),
        ],
        name="analysis",
    )(*in_vmem(*received, message))


def place_kernel(self_ref, got_ref, from_1, from_2, from_3, out_hbm, sem):
    member = lax.axis_index("member")
    row, core = member // 2, member % 2
    copies = []
    pieces = [self_ref, got_ref.at[0]]
    for ref in (from_1, from_2, from_3):
        pieces += [ref.at[0], ref.at[1]]
    for i, piece in enumerate(pieces):
        patch = (row + i // 2) % SHIFTS * 2 + (core + i) % 2
        lanes = pl.ds(pl.multiple_of(patch * PATCH_CELLS, PATCH_CELLS), PATCH_CELLS)
        copies.append(pltpu.make_async_copy(piece, out_hbm.at[:, lanes], sem.at[i]))
    for copy in copies:
        copy.start()
    for copy in copies:
        copy.wait()


def place(received, cells):
    rows = received[0].shape[0]
    return pl.pallas_call(
        place_kernel,
        out_shape=jax.ShapeDtypeStruct((rows, cells), jnp.bfloat16),
        in_specs=vmem(SHIFTS + 1),
        out_specs=pl.BlockSpec(memory_space=pltpu.HBM),
        scratch_shapes=[pltpu.SemaphoreType.DMA((2 * SHIFTS,))],
        compiler_params=pltpu.CompilerParams(vmem_limit_bytes=2 << 20),
        name="place",
    )(*in_vmem(*received))


def on_device(
    state, adjacent_columns, adjacent_rates, amplification_speed,
    obs_patch, obs_row, obs_value, obs_error,
):
    members, levels, cells = state.shape
    regions = lax.axis_size("region")
    groups = lax.axis_size("member")
    total = cells * regions
    flat = state.reshape(members * levels, cells)
    up_part, down_part, kept, coef, *observed = prepare(
        flat, adjacent_columns, adjacent_rates, amplification_speed[None, :],
        obs_patch[None, :], obs_row[None, :], obs_value[None, :], obs_error[None, :], total,
    )
    up = [(i, (i + 1) % regions) for i in range(regions)]
    left = lax.ppermute(up_part, "region", up)
    right = lax.ppermute(down_part, "region", [(j, i) for i, j in up])
    message = observation_message(*observed, regions, groups)
    message = lax.all_to_all(message, ("member", "region"), 0, 0, tiled=True)
    own = own_matrices(coef)
    parts = forecast(kept, left, right, own, right_matrices(right), coef)
    received = exchange(parts, 1)
    parts = analysis(received, message)
    back = exchange(parts, -1)
    return place(back, cells).reshape(members, levels, cells)


def solution(mesh):
    placed = (
        P("member", None, "region"),
        P(None, "region"),
        P(None, "region"),
        P("region"),
        P(("member", "region")),
        P(("member", "region")),
        P(("member", "region")),
        P(("member", "region")),
    )

    return jax.shard_map(
        on_device, mesh=mesh, in_specs=placed, out_specs=P("member", None, "region"), check_vma=False
    )
```

```python
import functools
import math

import jax
import jax.numpy as jnp
from jax import lax
from jax.experimental import pallas as pl
from jax.experimental.pallas import tpu as pltpu
from jax.sharding import PartitionSpec as P


PATCH_CELLS = 128
RIM = 256
STEPS = 3
NS_ITERS = 6
LEVELS = 8
BLOCK = 256
WINDOW = BLOCK + 2 * RIM
HALO = STEPS * RIM
COEF_ROWS = 16
TILE = 128
STATE_CHUNKS = 4
SHIFTS = 4
REST = (0, 1, 3)


def high(value):
    return value.astype(jnp.bfloat16)


def low(value):
    return (value - high(value).astype(jnp.float32)).astype(jnp.bfloat16)


def dot_f32(a, b, dims=(((1,), (0,)), ((), ()))):
    return lax.dot_general(a, b, dims, preferred_element_type=jnp.float32)


def dot_half(a, b, dims=(((1,), (0,)), ((), ()))):
    return dot_f32(high(a), high(b), dims)


def cell_offsets(columns, first, total):
    cell = first + lax.broadcasted_iota(jnp.int32, columns.shape, 1)
    offset = columns - cell
    offset = jnp.where(offset > total // 2, offset - total, offset)
    return jnp.where(offset < -(total // 2), offset + total, offset)


def matrix_tiles(matrix_ref, index, offsets, rates):
    offset = [offsets[k : k + 1] for k in range(6)]
    rate = [rates[k : k + 1] for k in range(6)]
    for k in range(6):
        for later in range(k + 1, 6):
            same = offset[later] == offset[k]
            rate[k] = rate[k] + jnp.where(same, rate[later], 0.0)
            offset[later] = jnp.where(same, float(-4 * RIM), offset[later])
    zero = jnp.zeros((TILE, TILE), jnp.bfloat16)
    row = lax.broadcasted_iota(jnp.int32, (TILE, TILE), 0).astype(jnp.float32)
    row = row.astype(jnp.bfloat16)
    lane = lax.broadcasted_iota(jnp.int32, (1, TILE), 1).astype(jnp.float32)
    reach = (TILE + 2 * RIM) // TILE
    steps = []
    for part in range(BLOCK // TILE):
        lanes = slice(part * TILE, (part + 1) * TILE)
        local = [item[:, lanes] + (lane + float(RIM)) for item in offset]
        spread = [item[:, lanes].astype(jnp.bfloat16) for item in rate]
        for tile in range(WINDOW // TILE):

            def write(tile=tile, part=part, lanes=lanes, local=local, spread=spread):
                rows = slice(tile * TILE, (tile + 1) * TILE)
                step = tile - part
                total = zero
                if 0 <= step < reach:
                    for k in range(6):
                        near = (local[k] - float(step * TILE)).astype(jnp.bfloat16)
                        hit = row == jnp.broadcast_to(near, (TILE, TILE))
                        total = jnp.where(hit, jnp.broadcast_to(spread[k], (TILE, TILE)), total)
                matrix_ref[index, rows, lanes] = total

            steps.append(write)
    return steps


def build_matrix(matrix_ref, index, offsets, rates):
    for step in matrix_tiles(matrix_ref, index, offsets, rates):
        step()


def fetches(sources, targets, sem):
    return [
        pltpu.make_async_copy(source, target, sem.at[i])
        for i, (source, target) in enumerate(zip(sources, targets))
    ]


def prepare_kernel(
    state_hbm, column_hbm, rate_hbm, speed_hbm, patch_hbm, row_hbm, value_hbm, error_hbm,
    up_ref, down_ref, state_ref, coef_ref, patch_ref, row_ref, value_ref, error_ref,
    column_ref, rate_ref, speed_ref, small_sem, later_sem, state_sem, *, total,
):
    rows, cells = state_ref.shape
    small = fetches(
        (column_hbm, rate_hbm, speed_hbm), (column_ref, rate_ref, speed_ref), small_sem
    )
    later = fetches(
        (patch_hbm, row_hbm, value_hbm, error_hbm),
        (patch_ref, row_ref, value_ref, error_ref),
        later_sem,
    )
    chunk = rows // STATE_CHUNKS
    large = [
        pltpu.make_async_copy(
            state_hbm.at[pl.ds(i * chunk, chunk)],
            state_ref.at[pl.ds(i * chunk, chunk)],
            state_sem.at[i],
        )
        for i in range(STATE_CHUNKS)
    ]
    for copy in small + large + later:
        copy.start()
    for copy in small:
        copy.wait()
    region = lax.axis_index("region")
    last = cells - HALO
    offsets = cell_offsets(column_ref[...], region * cells, total).astype(jnp.float32)
    rates = rate_ref[...]
    rate_sum = jnp.sum(rates, axis=0, keepdims=True)
    speed = speed_ref[...]
    coef_ref[...] = jnp.concatenate(
        [
            offsets,
            rates,
            high(rate_sum).astype(jnp.float32),
            low(rate_sum).astype(jnp.float32),
            high(speed).astype(jnp.float32),
            low(speed).astype(jnp.float32),
        ],
        axis=0,
    )
    up_ref[rows:] = coef_ref[:, last:].astype(jnp.bfloat16)
    down_ref[rows:] = coef_ref[:, :HALO].astype(jnp.bfloat16)
    for i, copy in enumerate(large):
        copy.wait()
        part = pl.ds(i * chunk, chunk)
        up_ref[part] = state_ref[part, last:].astype(jnp.bfloat16)
        down_ref[part] = state_ref[part, :HALO].astype(jnp.bfloat16)
    for copy in later:
        copy.wait()


def vmem(count):
    return [pl.BlockSpec(memory_space=pltpu.VMEM)] * count


def in_vmem(*values):
    return [pltpu.with_memory_space_constraint(value, pltpu.VMEM) for value in values]


def in_hbm(*values):
    return [pltpu.with_memory_space_constraint(value, pltpu.HBM) for value in values]


def prepare(state, columns, rates, speed, patch, row, value, error, total):
    rows, cells = state.shape
    side = pltpu.VMEM((rows + COEF_ROWS, HALO), jnp.bfloat16)
    return pl.pallas_call(
        functools.partial(prepare_kernel, total=total),
        out_shape=(
            side,
            side,
            pltpu.VMEM((rows, cells), jnp.float32),
            pltpu.VMEM((COEF_ROWS, cells), jnp.float32),
            *(pltpu.VMEM(item.shape, item.dtype) for item in (patch, row, value, error)),
        ),
        in_specs=[pl.BlockSpec(memory_space=pltpu.HBM)] * 8,
        out_specs=tuple(vmem(8)),
        scratch_shapes=[
            pltpu.VMEM(columns.shape, jnp.int32),
            pltpu.VMEM(rates.shape, jnp.float32),
            pltpu.VMEM(speed.shape, jnp.float32),
            pltpu.SemaphoreType.DMA((3,)),
            pltpu.SemaphoreType.DMA((4,)),
            pltpu.SemaphoreType.DMA((STATE_CHUNKS,)),
        ],
        compiler_params=pltpu.CompilerParams(vmem_limit_bytes=8 << 20),
        name="prepare",
    )(*in_hbm(state, columns, rates, speed, patch, row, value, error))


def matrices_kernel(coef_ref, state_ref, matrix_ref, inner_ref):
    blocks = matrix_ref.shape[0]
    for b in range(blocks):
        part = slice(b * BLOCK, (b + 1) * BLOCK)
        build_matrix(matrix_ref, b, coef_ref[0:6, part], coef_ref[6:12, part])
    for b in range(1, blocks - 1):
        part = slice(b * BLOCK, (b + 1) * BLOCK)
        window = state_ref[:, part.start - RIM : part.stop + RIM].astype(jnp.bfloat16)
        summed = dot_f32(window, matrix_ref[b])
        keep = 1.0 - (coef_ref[12:13, part] + coef_ref[13:14, part])
        blended = state_ref[:, part] * keep + summed
        quick = coef_ref[14:15, part] + coef_ref[15:16, part]
        inner_ref[:, part.start - RIM : part.stop - RIM] = blended + quick * jnp.tanh(blended)


def own_matrices(coef, state):
    rows, cells = state.shape
    return pl.pallas_call(
        matrices_kernel,
        out_shape=(
            pltpu.VMEM((cells // BLOCK, WINDOW, BLOCK), jnp.bfloat16),
            pltpu.VMEM((rows, cells - 2 * RIM), jnp.float32),
        ),
        in_specs=vmem(2),
        out_specs=tuple(vmem(2)),
        compiler_params=pltpu.CompilerParams(vmem_limit_bytes=4 << 20),
        name="own_matrices",
    )(*in_vmem(coef, state))


def right_kernel(right_ref, matrix_ref):
    rows = right_ref.shape[0] - COEF_ROWS
    for b in range(matrix_ref.shape[0]):
        part = slice(b * BLOCK, (b + 1) * BLOCK)
        coef = right_ref[rows:, part].astype(jnp.float32)
        build_matrix(matrix_ref, b, coef[0:6], coef[6:12])


def right_matrices(right):
    shape = ((STEPS - 1) * RIM // BLOCK, WINDOW, BLOCK)
    return pl.pallas_call(
        right_kernel,
        out_shape=pltpu.VMEM(shape, jnp.bfloat16),
        in_specs=vmem(1),
        out_specs=vmem(1)[0],
        compiler_params=pltpu.CompilerParams(vmem_limit_bytes=3 << 20),
        name="right_matrices",
    )(*in_vmem(right))


def message_kernel(patch_ref, row_ref, value_ref, error_ref, message_ref, *, regions, groups):
    devices, count = message_ref.shape[0], patch_ref.shape[1]
    target = lax.broadcasted_iota(jnp.int32, (devices, count), 0)
    wanted = target % regions * groups + target // regions
    hit = jnp.where(patch_ref[...] == wanted, 1.0, 0.0)
    before = lax.broadcasted_iota(jnp.int32, (count, count), 0)
    after = lax.broadcasted_iota(jnp.int32, (count, count), 1)
    earlier = jnp.where(before < after, 1.0, 0.0).astype(jnp.bfloat16)
    rank = dot_f32(hit.astype(jnp.bfloat16), earlier)
    field = lax.broadcasted_iota(jnp.int32, (message_ref.shape[1], count), 0)
    location = row_ref[...].astype(jnp.float32) + 1.0
    weight = 1.0 / (error_ref[...] * error_ref[...])
    message = None
    for slot in range(2):
        chosen = jnp.where(rank == float(slot), hit, 0.0).astype(jnp.bfloat16)
        values = jnp.zeros(field.shape, jnp.float32)
        for k, item in enumerate((location, value_ref[...], weight)):
            values = jnp.where(field == 3 * slot + k, item, values)
        for _ in range(3):
            piece = high(values)
            values = values - piece.astype(jnp.float32)
            term = dot_f32(chosen, piece, (((1,), (1,)), ((), ())))
            message = term if message is None else message + term
    message_ref[...] = message


def observation_message(patch, row, value, error, regions, groups):
    return pl.pallas_call(
        functools.partial(message_kernel, regions=regions, groups=groups),
        out_shape=jax.ShapeDtypeStruct((regions * groups, TILE), jnp.float32),
        in_specs=vmem(4),
        out_specs=vmem(1)[0],
        compiler_params=pltpu.CompilerParams(vmem_limit_bytes=4 << 20),
        name="message",
    )(*in_vmem(patch, row, value, error))


def forecast_kernel(
    state_ref, left_ref, right_ref, own_ref, side_ref, own_coef_ref, inner_ref, own_0, own_1, own_2, own_3,
    first_swap, rest_swap, matrix_ref, coef_ref, field_a, field_b, wide_ref,
):
    rows, cells = state_ref.shape
    own_blocks = cells // BLOCK
    side_blocks = (STEPS - 1) * RIM // BLOCK
    blocks = own_blocks + 2 * side_blocks
    far = HALO + cells
    for ref, begin in ((left_ref, 0), (right_ref, far)):
        coef_ref[:, begin : begin + HALO] = ref[rows:].astype(jnp.float32)
        field_a[:, begin : begin + HALO] = ref[:rows]
    coef_ref[:, HALO:far] = own_coef_ref[...]
    field_a[:, HALO:far] = state_ref[...].astype(jnp.bfloat16)
    keep, speed, matrices = [], [], []
    for b in range(blocks):
        part = slice(RIM + b * BLOCK, RIM + (b + 1) * BLOCK)
        if b >= side_blocks + own_blocks:
            matrices.append((side_ref, b - side_blocks - own_blocks))
        elif b >= side_blocks:
            matrices.append((own_ref, b - side_blocks))
        else:
            build_matrix(matrix_ref, b, coef_ref[0:6, part], coef_ref[6:12, part])
            matrices.append((matrix_ref, b))
        keep.append(1.0 - (coef_ref[12:13, part] + coef_ref[13:14, part]))
        speed.append(coef_ref[14:15, part] + coef_ref[15:16, part])
    source, target = field_a, field_b
    for step in range(STEPS - 1):
        for b in range(step, blocks - step):
            first = b * BLOCK
            middle = slice(first + RIM, first + RIM + BLOCK)
            if step == 0 and side_blocks < b < side_blocks + own_blocks - 1:
                start = (b - side_blocks) * BLOCK - RIM
                result = inner_ref[:, start : start + BLOCK]
                wide_ref[:, middle] = result
                target[:, middle] = result.astype(jnp.bfloat16)
                continue
            holder, index = matrices[b]
            summed = dot_f32(source[:, first : first + WINDOW], holder[index])
            if step > 0:
                centre = wide_ref[:, middle]
            elif side_blocks <= b < side_blocks + own_blocks:
                own = (b - side_blocks) * BLOCK
                centre = state_ref[:, own : own + BLOCK]
            else:
                centre = source[:, middle].astype(jnp.float32)
            blended = centre * keep[b] + summed
            result = blended + speed[b] * jnp.tanh(blended)
            wide_ref[:, middle] = result
            target[:, middle] = result.astype(jnp.bfloat16)
        source, target = target, source
    member = lax.axis_index("member")
    row, core = member // 2, member % 2
    for shift, own_out in enumerate((own_0, own_1, own_2, own_3)):
        block = (row + shift) % own_blocks
        first = pl.multiple_of(block * BLOCK + (HALO - RIM), TILE)
        middle = pl.ds(pl.multiple_of(block * BLOCK + HALO, TILE), BLOCK)
        summed = dot_f32(source[:, pl.ds(first, WINDOW)], own_ref[block])
        kept = 1.0 - (coef_ref[12:13, middle] + coef_ref[13:14, middle])
        quick = coef_ref[14:15, middle] + coef_ref[15:16, middle]
        blended = wide_ref[:, middle] * kept + summed
        result = (blended + quick * jnp.tanh(blended)).astype(jnp.bfloat16)
        even, odd_half = result[:, :PATCH_CELLS], result[:, PATCH_CELLS:]
        own_out[...] = jnp.where(core == 0, even, odd_half)
        store_swap(shift, jnp.where(core == 0, odd_half, even), first_swap, rest_swap)


def exchange_shapes(rows):
    return (pltpu.VMEM((rows, PATCH_CELLS), jnp.bfloat16),) * (SHIFTS + 1) + (
        pltpu.VMEM((len(REST), rows, PATCH_CELLS), jnp.bfloat16),
    )


def store_swap(shift, value, first_ref, rest_ref):
    if shift in REST:
        rest_ref[REST.index(shift)] = value
    else:
        first_ref[...] = value


def forecast(state, left, right, own, side, coef, inner):
    rows, cells = state.shape
    sides = (STEPS - 1) * RIM // BLOCK
    padded = cells + 2 * HALO
    return pl.pallas_call(
        forecast_kernel,
        out_shape=exchange_shapes(rows),
        in_specs=vmem(7),
        out_specs=tuple(vmem(SHIFTS + 2)),
        scratch_shapes=[
            pltpu.VMEM((sides, WINDOW, BLOCK), jnp.bfloat16),
            pltpu.VMEM((COEF_ROWS, padded), jnp.float32),
            pltpu.VMEM((rows, padded), jnp.bfloat16),
            pltpu.VMEM((rows, padded), jnp.bfloat16),
            pltpu.VMEM((rows, padded), jnp.float32),
        ],
        compiler_params=pltpu.CompilerParams(vmem_limit_bytes=16 << 20),
        name="forecast",
    )(*in_vmem(state, left, right, own, side, coef, inner))


def merge_kernel(own_2, got_ref, out_2):
    out_2[0] = own_2[...]
    out_2[1] = got_ref[...]


def merge_rest_kernel(own_1, own_3, got_ref, out_1, out_3):
    for shift, own, out in ((1, own_1, out_1), (3, own_3, out_3)):
        out[0] = own[...]
        out[1] = got_ref[REST.index(shift)]


def merge(kernel, *parts):
    rows = parts[0].shape[0]
    count = len(parts) - 1
    return pl.pallas_call(
        kernel,
        out_shape=(pltpu.VMEM((2, rows, PATCH_CELLS), jnp.bfloat16),) * count,
        in_specs=vmem(count + 1),
        out_specs=tuple(vmem(count)),
        compiler_params=pltpu.CompilerParams(vmem_limit_bytes=2 << 20),
    )(*in_vmem(*parts))


def exchange(parts, sign):
    groups = lax.axis_size("member")
    swap = [(i, i ^ 1) for i in range(groups)]
    *own, first_swap, rest_swap = parts
    got_first = lax.ppermute(first_swap, "member", swap)
    got_rest = lax.ppermute(rest_swap, "member", swap)
    (merged_2,) = merge(merge_kernel, own[2], got_first)
    merged_1, merged_3 = merge(merge_rest_kernel, own[1], own[3], got_rest)
    moved = {}
    for shift, merged in ((2, merged_2), (1, merged_1), (3, merged_3)):
        edges = [(i, (i + sign * 2 * shift) % groups) for i in range(groups)]
        moved[shift] = lax.ppermute(merged, "member", edges)
    return own[0], got_rest, moved[1], moved[2], moved[3]


def analysis_kernel(
    self_ref, got_ref, from_1, from_2, from_3, message_ref, own_0, own_1, own_2, own_3,
    first_swap, rest_swap, wide_ref, x2_ref, select_ref,
):
    rows = self_ref.shape[0]
    members = wide_ref.shape[0] // LEVELS
    span = LEVELS * PATCH_CELLS
    arrived = [self_ref[...], got_ref[0]]
    for ref in (from_1, from_2, from_3):
        arrived += [ref[0], ref[1]]
    for i, piece in enumerate(arrived):
        wide_ref[i * rows : (i + 1) * rows] = piece.astype(jnp.float32)
    for level in range(LEVELS):
        part = wide_ref[pl.ds(level, members, stride=LEVELS), :]
        x2_ref[:, level * PATCH_CELLS : (level + 1) * PATCH_CELLS] = part.astype(jnp.bfloat16)
    message = jnp.transpose(message_ref[...])
    location = jnp.concatenate([message[0:1], message[3:4]], axis=1) - 1.0
    value = jnp.concatenate([message[1:2], message[4:5]], axis=1)
    weight = jnp.concatenate([message[2:3], message[5:6]], axis=1)
    slots = location.shape[1]
    location = location.astype(jnp.int32)
    for first in range(0, span, PATCH_CELLS):
        row = lax.broadcasted_iota(jnp.int32, (PATCH_CELLS, slots), 0) + first
        hot = jnp.where(row == location, 1.0, 0.0)
        select_ref[first : first + PATCH_CELLS, :] = hot.astype(jnp.bfloat16)
    seen = dot_f32(x2_ref[...], select_ref[...])
    seen_mean = jnp.sum(seen, axis=0, keepdims=True) * (1.0 / members)
    rooted = jnp.sqrt(weight)
    spread = 1.0 / math.sqrt(members - 1.0)
    scaled = (seen - seen_mean) * (rooted * spread)
    row = lax.broadcasted_iota(jnp.int32, (members, members), 0)
    column = lax.broadcasted_iota(jnp.int32, (members, members), 1)
    diagonal = jnp.where(row == column, 1.0, 0.0)
    product = dot_half(scaled, scaled, (((1,), (1,)), ((), ())))
    system = diagonal + product
    square = jnp.sum(jnp.sum(system * system, axis=0, keepdims=True), axis=1, keepdims=True)
    inverse_scale = jnp.broadcast_to(lax.rsqrt(square), (1, members))
    innovation = rooted * (value - seen_mean) * spread
    forcing = jnp.sum(scaled * innovation, axis=1, keepdims=True)
    p, z = inverse_scale, jnp.ones_like(inverse_scale)
    both = product * inverse_scale
    root = None
    for sweep in range(NS_ITERS):
        f = 1.5 - 0.5 * p
        factor = -0.5 * both
        narrow = factor.astype(jnp.bfloat16)
        if root is None:
            new_root = factor
        else:
            new_root = z * factor + f * root
        if sweep < NS_ITERS - 1:
            once = p * factor + f * both
            if root is None:
                once = once + dot_f32(high(both), narrow)
            else:
                stacked = dot_f32(jnp.concatenate([high(both), high(root)], axis=0), narrow)
                once = once + stacked[:members]
                new_root = new_root + stacked[members:]
            q = p * f
            both = q * factor + f * once + dot_f32(high(once), narrow)
            p = q * f
        else:
            new_root = new_root + dot_f32(high(root), narrow)
        root, z = new_root, z * f
    whole = root + z * diagonal
    inner = jnp.sum(whole * forcing, axis=0, keepdims=True)
    shift = jnp.sum(whole * inner, axis=1, keepdims=True) * inverse_scale[:, 0:1]
    half_scale = jnp.sqrt(inverse_scale)
    transform = (root * half_scale).astype(jnp.bfloat16)
    direct = (z * half_scale)[:, 0:PATCH_CELLS]
    pair = 2
    for level in range(0, LEVELS, pair):
        pieces = []
        for k in range(level, level + pair):
            part = x2_ref[:, k * PATCH_CELLS : (k + 1) * PATCH_CELLS].astype(jnp.float32)
            mean = jnp.sum(part, axis=0, keepdims=True) * (1.0 / members)
            anomaly = part - mean
            base = mean + jnp.sum(anomaly * shift, axis=0, keepdims=True) + direct * anomaly
            pieces.append((anomaly.astype(jnp.bfloat16), base))
        moved = dot_f32(transform, jnp.concatenate([piece[0] for piece in pieces], axis=1))
        for k in range(pair):
            updated = pieces[k][1] + moved[:, k * PATCH_CELLS : (k + 1) * PATCH_CELLS]
            wide_ref[pl.ds(level + k, members, stride=LEVELS), :] = updated
    for shift, own in enumerate((own_0, own_1, own_2, own_3)):
        first = 2 * shift * rows
        own[...] = wide_ref[first : first + rows].astype(jnp.bfloat16)
        other = wide_ref[first + rows : first + 2 * rows].astype(jnp.bfloat16)
        store_swap(shift, other, first_swap, rest_swap)


def analysis(received, message):
    rows = received[0].shape[0]
    wide = 2 * SHIFTS * rows
    members = wide // LEVELS
    slots = 2 * message.shape[0]
    return pl.pallas_call(
        analysis_kernel,
        out_shape=exchange_shapes(rows),
        in_specs=vmem(SHIFTS + 2),
        out_specs=tuple(vmem(SHIFTS + 2)),
        compiler_params=pltpu.CompilerParams(vmem_limit_bytes=12 << 20),
        scratch_shapes=[
            pltpu.VMEM((wide, PATCH_CELLS), jnp.float32),
            pltpu.VMEM((members, LEVELS * PATCH_CELLS), jnp.bfloat16),
            pltpu.VMEM((LEVELS * PATCH_CELLS, slots), jnp.bfloat16),
        ],
        name="analysis",
    )(*in_vmem(*received, message))


def place_kernel(self_ref, got_ref, from_1, from_2, from_3, out_hbm, sem):
    member = lax.axis_index("member")
    row, core = member // 2, member % 2
    copies = []
    pieces = [self_ref, got_ref.at[0]]
    for ref in (from_1, from_2, from_3):
        pieces += [ref.at[0], ref.at[1]]
    for i, piece in enumerate(pieces):
        patch = (row + i // 2) % SHIFTS * 2 + (core + i) % 2
        lanes = pl.ds(pl.multiple_of(patch * PATCH_CELLS, PATCH_CELLS), PATCH_CELLS)
        copies.append(pltpu.make_async_copy(piece, out_hbm.at[:, lanes], sem.at[i]))
    for copy in copies:
        copy.start()
    for copy in copies:
        copy.wait()


def place(received, cells):
    rows = received[0].shape[0]
    return pl.pallas_call(
        place_kernel,
        out_shape=jax.ShapeDtypeStruct((rows, cells), jnp.bfloat16),
        in_specs=vmem(SHIFTS + 1),
        out_specs=pl.BlockSpec(memory_space=pltpu.HBM),
        scratch_shapes=[pltpu.SemaphoreType.DMA((2 * SHIFTS,))],
        compiler_params=pltpu.CompilerParams(vmem_limit_bytes=2 << 20),
        name="place",
    )(*in_vmem(*received))


def on_device(
    state, adjacent_columns, adjacent_rates, amplification_speed,
    obs_patch, obs_row, obs_value, obs_error,
):
    members, levels, cells = state.shape
    regions = lax.axis_size("region")
    groups = lax.axis_size("member")
    total = cells * regions
    flat = state.reshape(members * levels, cells)
    up_part, down_part, kept, coef, *observed = prepare(
        flat, adjacent_columns, adjacent_rates, amplification_speed[None, :],
        obs_patch[None, :], obs_row[None, :], obs_value[None, :], obs_error[None, :], total,
    )
    up = [(i, (i + 1) % regions) for i in range(regions)]
    left = lax.ppermute(up_part, "region", up)
    right = lax.ppermute(down_part, "region", [(j, i) for i, j in up])
    message = observation_message(*observed, regions, groups)
    message = lax.all_to_all(message, ("member", "region"), 0, 0, tiled=True)
    own, inner = own_matrices(coef, kept)
    parts = forecast(kept, left, right, own, right_matrices(right), coef, inner)
    received = exchange(parts, 1)
    parts = analysis(received, message)
    back = exchange(parts, -1)
    return place(back, cells).reshape(members, levels, cells)


def solution(mesh):
    placed = (
        P("member", None, "region"),
        P(None, "region"),
        P(None, "region"),
        P("region"),
        P(("member", "region")),
        P(("member", "region")),
        P(("member", "region")),
        P(("member", "region")),
    )

    return jax.shard_map(
        on_device, mesh=mesh, in_specs=placed, out_specs=P("member", None, "region"), check_vma=False
    )
```
